128 devices in a mesh: dp: 8 (over y, x_lo), tp: 16 (over z, x_hi, core).
Axes of the slice: x: 4 (x_hi: 2, x_lo: 2; x = x_hi * 2 + x_lo), y: 4, z: 4, core: 2. Of those that a mesh axis runs over, the one named last changes fastest.
Arguments:
- gradients: bfloat16 [8, 4, 3072, 768], P('dp', None, 'tp'), may hold values from -6 to 6, as said below
- right_factor: float32 [4, 768, 8], replicated, may hold values from -6 to 6
- weights_before: float32 [4, 3072, 768], P(None, 'tp', 'dp'), may hold values from -0.21875 to 0.21875
- momentum: float32 [4, 3072, 768], P(None, 'tp', 'dp'), may hold values from -0.3125 to 0.3125
Outputs:
- new_weights: float32 [4, 3072, 768], P(None, 'tp', 'dp')
- new_basis: float32 [4, 768, 8], replicated
- new_momentum: float32 [4, 3072, 768], P(None, 'tp', 'dp')
The draws below stay inside these ranges and needn't reach their ends.
Inputs may be any that keep to these rules, and one draw needn't show every extreme that they name: gradients holds numbers from -6 to 6.
All inputs are finite; a program needn't handle non-finite values.
Results may differ from the reference program's by a relative error of at most 0.0003.
Values sent between devices are 32-bit elements.
A program may use at most 64 MiB of HBM per device.

```python
import jax
import jax.numpy as jnp
from jax import lax

WIDTH = 768
INNER = 3072
RANK = 8
LAYERS = 4
REPLICAS = 8
N_TP = 16


def draw_gradients(key, part):
    keys = jax.random.split(key, 5)
    level = jnp.exp(jax.random.uniform(keys[4], (1, LAYERS, N_TP, 1, RANK), jnp.float32, -1.3, 1.3))
    left = jax.random.normal(keys[0], (1, LAYERS, N_TP, INNER // N_TP, RANK), jnp.float32) * level
    left = left.reshape(1, LAYERS, INNER, RANK)
    right = jax.random.normal(keys[1], (1, LAYERS, RANK, WIDTH), jnp.float32)
    strength = jax.random.normal(keys[2], (REPLICAS, LAYERS, 1, RANK), jnp.float32)
    noise = jax.random.normal(keys[3], (REPLICAS, LAYERS, INNER, WIDTH), jnp.float32)
    low = jnp.einsum('alir,lrw->aliw', left * strength, right[0])
    values = low * RANK ** (-0.5) + 0.5 * noise
    return jnp.clip(values, -6.0, 6.0).astype(jnp.bfloat16)


def levels(own_key, shape, pieces, smallest, high):
    gain, own = 1.0, jax.random.fold_in(own_key, 6)
    for position, shards_of in pieces:
        steps = jnp.exp(jax.random.uniform(jax.random.fold_in(own, position), (shards_of,), jnp.float32, smallest / len(pieces), high / len(pieces)))
        gain = gain * jnp.repeat(steps, shape[position] // shards_of).reshape([-1 if axis == position else 1 for axis in range(len(shape))])
    return gain


def gaussian(stream_key, shape, spread, bound, cuts=(), held_as=jnp.bfloat16):
    gain = levels(stream_key, shape, cuts, -0.22, 0.18) if cuts else 1.0
    values = jax.random.normal(stream_key, shape, jnp.float32) * spread * gain
    return jnp.minimum(jnp.maximum(values, -bound), bound).astype(held_as)


def setup_inputs(seed: int = 0) -> dict:
    splits = jax.random.split(jax.random.key(seed), 5)
    return {
        "gradients": draw_gradients(jax.random.fold_in(splits[4], 71), 0),
        "right_factor": gaussian(splits[1], (LAYERS, WIDTH, RANK), 1.0, 6.0, (), jnp.float32),
        "weights_before": gaussian(splits[2], (LAYERS, INNER, WIDTH), WIDTH ** -0.5, 0.21875, ((1, 16), (2, 8)), jnp.float32),
        "momentum": gaussian(splits[3], (LAYERS, INNER, WIDTH), 0.05, 0.3125, ((1, 16), (2, 8)), jnp.float32),
    }


def reference(gradients, right_factor, weights_before, momentum):
    small_basis = right_factor.astype(jnp.bfloat16)
    small_basis = lax.optimization_barrier(small_basis)
    left = jnp.einsum('aliw,lwr->lir', gradients.astype(jnp.float32), small_basis.astype(jnp.float32))
    gram = jnp.einsum('lir,lis->lrs', left, left, precision=lax.Precision.HIGHEST)
    gram = gram + 0.001 * lax.optimization_barrier(jnp.mean(jnp.diagonal(gram, axis1=1, axis2=2), axis=1))[:, None, None] * jnp.eye(RANK, dtype=jnp.float32)
    small_left = lax.optimization_barrier(left.astype(jnp.bfloat16))
    right = jnp.einsum('aliw,lir->lwr', gradients.astype(jnp.float32), small_left.astype(jnp.float32))
    root = jnp.linalg.cholesky(gram)
    half = lax.linalg.triangular_solve(root, jnp.swapaxes(right, 1, 2), left_side=True, lower=True)
    mixed = lax.linalg.triangular_solve(root, half, left_side=True, lower=True, transpose_a=True)
    change = jnp.einsum('lir,lrw->liw', left, mixed, precision=lax.Precision.HIGHEST) / REPLICAS
    new_momentum = 0.9 * momentum + change
    new_weights = weights_before - 0.02 * new_momentum
    new_basis = right * lax.rsqrt(lax.optimization_barrier(jnp.mean(right * right, axis=(1, 2), keepdims=True)) + 1e-12)
    return (new_weights, new_basis, new_momentum)
```

```python
import functools

import jax
import jax.numpy as jnp
from jax import lax
from jax.experimental import pallas as pl
from jax.experimental.pallas import tpu as pltpu
from jax.sharding import PartitionSpec as P

MESH = pl.DeviceIdType.MESH
LANES = 128


def split3(x):
    high = x.astype(jnp.bfloat16).astype(jnp.float32)
    rest = x - high
    mid = rest.astype(jnp.bfloat16).astype(jnp.float32)
    low = (rest - mid).astype(jnp.bfloat16).astype(jnp.float32)
    return high, mid, low


def kernel(
    ndp, ntp, grads, basis, weights, momentum,
    out_weights, out_basis, out_momentum,
    b_buf, g_buf, w_buf, m_buf, lefts, grams, rights, parts, full, y_buf,
    g_sem, wm_sem, left_send, left_recv, gram_send, gram_recv, part_send, part_recv, full_send, full_recv,
):
    layers, rank, rows = lefts.shape[0], lefts.shape[2], lefts.shape[3]
    width = grads.shape[2]
    columns = weights.shape[2]
    n = ndp * ntp
    tiles = width // LANES
    pieces = layers * tiles
    my_dp, my_tp = lax.axis_index("dp"), lax.axis_index("tp")
    me = my_dp * ntp + my_tp

    group = -(-pieces // ndp)
    span = max(
        ((d + 1) * columns - 1) // LANES - d * columns // LANES + 1 for d in range(ndp)
    )

    def device(flat):
        return (flat // ntp, lax.rem(flat, ntp))

    def owner_of(l, t):
        place = t * layers + l
        within = place % group
        tp = within * ntp // group if group <= ntp else within % ntp
        return place // group * ntp + tp

    def round_of(l, t):
        return 0 if group <= ntp else (t * layers + l) % group // ntp

    def first_tile(d, least=min):
        return least(d * columns // LANES, tiles - span)

    loads = [pltpu.make_async_copy(grads.at[l], g_buf.at[l], g_sem.at[l]) for l in range(layers)]
    for load in loads:
        load.start()
    basis_load = pltpu.make_async_copy(basis, b_buf, wm_sem.at[2])
    basis_load.start()
    state_loads = [
        pltpu.make_async_copy(weights, w_buf, wm_sem.at[0]),
        pltpu.make_async_copy(momentum, m_buf, wm_sem.at[1]),
    ]
    for load in state_loads:
        load.start()

    grams[my_tp] = jnp.zeros(grams.shape[1:], jnp.float32)
    barrier = pltpu.get_barrier_semaphore()
    for k in range(1, n):
        pl.semaphore_signal(barrier, inc=1, device_id=device(lax.rem(me + k, n)), device_id_type=MESH)

    def left_copy(l, k):
        return pltpu.make_async_remote_copy(
            src_ref=lefts.at[l, my_dp], dst_ref=lefts.at[l, my_dp],
            send_sem=left_send, recv_sem=left_recv.at[l],
            device_id=(lax.rem(my_dp + k, ndp), my_tp), device_id_type=MESH,
        )

    for l in range(layers):
        if l == 0:
            basis_load.wait()
        loads[l].wait()
        lefts[l, my_dp] = lax.dot_general(
            b_buf[l].astype(jnp.bfloat16), g_buf[l], (((1,), (1,)), ((), ())), preferred_element_type=jnp.float32
        )
    pl.semaphore_wait(barrier, n - 1)
    for l in range(layers):
        for k in range(1, ndp):
            left_copy(l, k).start()

    def part_copy(l, t):
        j, owner, turn = l * tiles + t, owner_of(l, t), round_of(l, t)
        return pltpu.make_async_remote_copy(
            src_ref=rights.at[j], dst_ref=parts.at[turn, me],
            send_sem=part_send, recv_sem=part_recv.at[turn],
            device_id=(owner // ntp, owner % ntp), device_id_type=MESH,
        )

    all_left = []
    for l in range(layers):
        if ndp > 1:
            landed = lefts.at[l, pl.ds(0, ndp - 1)]
            pltpu.make_async_copy(landed, landed, left_recv.at[l]).wait()
        left = lefts[l, 0]
        for d in range(1, ndp):
            left = left + lefts[l, d]
        all_left.append(left)
        right = jnp.dot(left.astype(jnp.bfloat16), g_buf[l], preferred_element_type=jnp.float32)
        for t in range(tiles):
            rights[l * tiles + t] = right[:, t * LANES:(t + 1) * LANES]
        for t in range(tiles):

            @pl.when(me != owner_of(l, t))
            def _():
                part_copy(l, t).start()

    stacked = jnp.concatenate(all_left, axis=0)
    products = lax.dot_general(
        stacked, stacked, (((1,), (1,)), ((), ())),
        precision=lax.Precision.HIGHEST, preferred_element_type=jnp.float32,
    )
    where = lax.broadcasted_iota(jnp.int32, (rank, layers * rank), 1) // rank
    packed = jnp.zeros((rank, layers * rank), jnp.float32)
    for l in range(layers):
        packed = jnp.where(where == l, products[l * rank:(l + 1) * rank], packed)
    grams[my_tp, :, :layers * rank] = packed

    def gram_copy(k):
        return pltpu.make_async_remote_copy(
            src_ref=grams.at[my_tp], dst_ref=grams.at[my_tp],
            send_sem=gram_send, recv_sem=gram_recv,
            device_id=(my_dp, lax.rem(my_tp + k, ntp)), device_id_type=MESH,
        )

    for k in range(1, ntp):
        gram_copy(k).start()

    every = [(l, t) for l in range(layers) for t in range(tiles)]

    def full_copies(l, t):
        j, owner = l * tiles + t, owner_of(l, t)
        others = [(d, p) for d in range(ndp) for p in range(ntp) if d * ntp + p != owner]
        others.sort(key=lambda x: (not 0 <= t - first_tile(x[0]) < span, -abs(x[1] - owner % ntp)))
        return [
            pltpu.make_async_remote_copy(
                src_ref=full.at[j], dst_ref=full.at[j],
                send_sem=full_send, recv_sem=full_recv.at[j],
                device_id=other, device_id_type=MESH,
            )
            for other in others
        ]

    for l, t in every:
        q, j = round_of(l, t), l * tiles + t

        @pl.when(me == owner_of(l, t))
        def _():
            landed = parts.at[q, pl.ds(0, n - 1)]
            pltpu.make_async_copy(landed, landed, part_recv.at[q]).wait()
            parts[q, me] = rights[j]
            full[j] = jnp.sum(parts[q], axis=0)
            for copy in full_copies(l, t):
                copy.start()

    if ntp > 1:
        landed = grams.at[pl.ds(0, ntp - 1)]
        pltpu.make_async_copy(landed, landed, gram_recv).wait()
    gram_sum = jnp.sum(grams[...], axis=0)
    line = lax.broadcasted_iota(jnp.int32, (rank, rank), 0)
    diagonal = line == lax.broadcasted_iota(jnp.int32, (rank, rank), 1)
    step_line = lax.broadcasted_iota(jnp.int32, (rank, 1), 0)
    systems = []
    for l in range(layers):
        gram = gram_sum[:, l * rank:(l + 1) * rank]
        ridge = 0.001 * (jnp.sum(jnp.where(diagonal, gram, 0.0)) / rank)
        systems.append((gram + jnp.where(diagonal, ridge, 0.0), all_left[l]))
    for k in range(rank):
        after = []
        for gram, y in systems:
            pivot = 1.0 / gram[k:k + 1, k:k + 1]
            gram_row, y_row = gram[k:k + 1] * pivot, y[k:k + 1] * pivot
            factor = gram[:, k:k + 1]
            here = step_line == k
            after.append((
                jnp.where(here, gram_row, gram - factor * gram_row),
                jnp.where(here, y_row, y - factor * y_row),
            ))
        systems = after
    for l in range(layers):
        high, mid, low = split3(systems[l][1] / ndp)
        y = jnp.concatenate([high, high, high, mid, mid, low], axis=0)
        y_buf[l] = y.T.astype(jnp.bfloat16)
    for load in state_loads:
        load.wait()

    def wait_full(j):
        pltpu.make_async_copy(full.at[j], full.at[j], full_recv.at[j]).wait()

    start = first_tile(my_dp, jnp.minimum)
    shift = lax.rem(span * LANES - (my_dp * columns - start * LANES), span * LANES)
    for l in range(layers):
        for i in range(span):
            t = start + i

            @pl.when(me != owner_of(l, t))
            def _():
                wait_full(l * tiles + t)
        near = jnp.concatenate([full[l * tiles + start + i] for i in range(span)], axis=1)
        own = pltpu.roll(near, shift, 1)[:, :columns]
        high, mid, low = split3(own)
        own = jnp.concatenate([high, mid, low, high, mid, high], axis=0).astype(jnp.bfloat16)
        change = jnp.dot(y_buf[l], own, preferred_element_type=jnp.float32)
        moved = 0.9 * m_buf[l] + change
        out_momentum[l] = moved
        out_weights[l] = w_buf[l] - 0.02 * moved

    for l in range(layers):
        for t in range(tiles):

            @pl.when((me != owner_of(l, t)) & ((t < start) | (t >= start + span)))
            def _():
                wait_full(l * tiles + t)
        right = jnp.concatenate([full[l * tiles + t] for t in range(tiles)], axis=1)
        out_basis[l] = right * lax.rsqrt(jnp.mean(right * right) + 1e-12)

    for l in range(layers):
        for k in range(1, ndp):
            left_copy(l, k).wait_send()
    for k in range(1, ntp):
        gram_copy(k).wait_send()
    for l, t in every:

        @pl.when(me != owner_of(l, t))
        def _():
            part_copy(l, t).wait_send()

        @pl.when(me == owner_of(l, t))
        def _():
            for copy in full_copies(l, t):
                copy.wait_send()


def writer(*refs):
    half = (len(refs) - 1) // 2
    copies = [pltpu.make_async_copy(refs[i], refs[half + i], refs[-1].at[i]) for i in range(half)]
    for copy in copies:
        copy.start()
    for copy in copies:
        copy.wait()


def solution(mesh):
    ndp, ntp = mesh.shape["dp"], mesh.shape["tp"]
    n = ndp * ntp

    def on_device(gradients, right_factor, weights_before, momentum):
        layers, rows, width = gradients.shape[1:]
        rank = right_factor.shape[2]
        columns = weights_before.shape[2]
        pieces = layers * (width // LANES)
        rounds = -(-(-(-pieces // ndp)) // ntp)
        basis = jnp.swapaxes(right_factor, 1, 2)
        f32 = jnp.float32
        keep = functools.partial(pltpu.with_memory_space_constraint, memory_space=pltpu.HBM)
        results = pl.pallas_call(
            functools.partial(kernel, ndp, ntp),
            out_shape=(
                jax.ShapeDtypeStruct((layers, rows, columns), f32),
                jax.ShapeDtypeStruct((layers, rank, width), f32),
                jax.ShapeDtypeStruct((layers, rows, columns), f32),
            ),
            in_specs=[
                pl.BlockSpec(memory_space=pltpu.HBM),
                pl.BlockSpec(memory_space=pltpu.HBM),
                pl.BlockSpec(memory_space=pltpu.HBM),
                pl.BlockSpec(memory_space=pltpu.HBM),
            ],
            out_specs=[pl.BlockSpec(memory_space=pltpu.VMEM)] * 3,
            scratch_shapes=[
                pltpu.VMEM((layers, rank, width), f32),
                pltpu.VMEM((layers, rows, width), jnp.bfloat16),
                pltpu.VMEM((layers, rows, columns), f32),
                pltpu.VMEM((layers, rows, columns), f32),
                pltpu.VMEM((layers, ndp, rank, rows), f32),
                pltpu.VMEM((ntp, rank, LANES), f32),
                pltpu.VMEM((pieces, rank, LANES), f32),
                pltpu.VMEM((rounds, n, rank, LANES), f32),
                pltpu.VMEM((pieces, rank, LANES), f32),
                pltpu.VMEM((layers, rows, 6 * rank), jnp.bfloat16),
                pltpu.SemaphoreType.DMA((layers,)),
                pltpu.SemaphoreType.DMA((3,)),
                pltpu.SemaphoreType.DMA,
                pltpu.SemaphoreType.DMA((layers,)),
                pltpu.SemaphoreType.DMA,
                pltpu.SemaphoreType.DMA,
                pltpu.SemaphoreType.DMA,
                pltpu.SemaphoreType.DMA((rounds,)),
                pltpu.SemaphoreType.DMA,
                pltpu.SemaphoreType.DMA((pieces,)),
            ],
            compiler_params=pltpu.CompilerParams(
                collective_id=0, has_side_effects=True, vmem_limit_bytes=24 * 1024 * 1024
            ),
        )(
            keep(gradients[0]), keep(basis),
            keep(weights_before), keep(momentum),
        )
        new_weights, new_basis, new_momentum = pl.pallas_call(
            writer,
            out_shape=tuple(jax.ShapeDtypeStruct(x.shape, x.dtype) for x in results),
            in_specs=[pl.BlockSpec(memory_space=pltpu.VMEM)] * 3,
            out_specs=[pl.BlockSpec(memory_space=pltpu.HBM)] * 3,
            scratch_shapes=[pltpu.SemaphoreType.DMA((3,))],
        )(*(pltpu.with_memory_space_constraint(x, pltpu.VMEM) for x in results))
        return new_weights, jnp.swapaxes(new_basis, 1, 2), new_momentum

    in_specs = (P("dp", None, "tp", None), P(), P(None, "tp", "dp"), P(None, "tp", "dp"))
    out_specs = (P(None, "tp", "dp"), P(), P(None, "tp", "dp"))
    return jax.shard_map(on_device, mesh=mesh, in_specs=in_specs, out_specs=out_specs, check_vma=False)
```

```python
import functools

import jax
import jax.numpy as jnp
from jax import lax
from jax.experimental import pallas as pl
from jax.experimental.pallas import tpu as pltpu
from jax.sharding import PartitionSpec as P

MESH = pl.DeviceIdType.MESH
LANES = 128


def split3(x):
    high = x.astype(jnp.bfloat16).astype(jnp.float32)
    rest = x - high
    mid = rest.astype(jnp.bfloat16).astype(jnp.float32)
    low = (rest - mid).astype(jnp.bfloat16).astype(jnp.float32)
    return high, mid, low


def pack(pair):
    whole = pair[0].shape[1] // LANES * LANES
    return jnp.concatenate([x[:, :whole] for x in pair] + [x[:, whole:] for x in pair], axis=1)


def unpack(x):
    rows = x.shape[1] // 2
    whole = rows // LANES * LANES
    rest = rows - whole
    return [
        jnp.concatenate(
            [x[:, i * whole:(i + 1) * whole], x[:, 2 * whole + i * rest:2 * whole + (i + 1) * rest]], axis=1
        )
        for i in range(2)
    ]


def owner_place(j):
    x_hi, y, z = j % 2, j // 2 % 4, j // 8
    return y * 2 + (y + z) % 2, z * 4 + x_hi * 2 + 1


def start_order(device):
    dp, tp = device
    x, y, z, core = tp // 2 % 2 * 2 + dp % 2, dp // 2, tp // 4, tp % 2
    return 10 * z + 6 * y + 4 * x + 5 * (1 - core)


def kernel(
    ndp, ntp, grads, basis, weights, momentum,
    out_weights, out_basis, out_momentum,
    b_buf, g_buf, w_buf, m_buf, lefts, grams, rights, parts, full, y_buf,
    g_sem, wm_sem, left_send, left_recv, gram_send, gram_recv, part_send, part_recv, full_send, full_recv,
):
    layers, rows, width = grads.shape
    rank = basis.shape[1]
    columns = weights.shape[2]
    n = ndp * ntp
    tiles = width // LANES
    pieces = layers * tiles
    my_dp, my_tp = lax.axis_index("dp"), lax.axis_index("tp")
    me = my_dp * ntp + my_tp

    span = max(
        ((d + 1) * columns - 1) // LANES - d * columns // LANES + 1 for d in range(ndp)
    )

    def first_tile(d, least=min):
        return least(d * columns // LANES, tiles - span)

    owners = [owner_place(j) for j in range(pieces)]
    devices = sorted(((d, p) for d in range(ndp) for p in range(ntp)), key=start_order)
    my_y, my_z = my_dp // 2, my_tp // 4
    owning = (
        (lax.rem(my_tp, 2) == 1) & (my_z * 8 < pieces) & (lax.rem(my_dp, 2) == lax.rem(my_y + my_z, 2))
    )
    my_piece = lax.min(my_z * 8 + my_y * 2 + lax.rem(my_tp // 2, 2), pieces - 1)
    my_layer = my_piece // tiles

    def is_me(device):
        return me == device[0] * ntp + device[1]

    def each_other(act):
        for device in devices:
            if device in owners:

                @pl.when(jnp.logical_not(is_me(device)))
                def _():
                    act(device)
            else:
                act(device)

    basis_load = pltpu.make_async_copy(basis, b_buf, wm_sem.at[2])
    basis_load.start()
    loads = [pltpu.make_async_copy(grads.at[l], g_buf.at[l], g_sem.at[l]) for l in range(layers)]
    for load in loads:
        load.start()
    state_loads = [
        pltpu.make_async_copy(weights, w_buf, wm_sem.at[0]),
        pltpu.make_async_copy(momentum, m_buf, wm_sem.at[1]),
    ]
    for load in state_loads:
        load.start()

    barrier = pltpu.get_barrier_semaphore()
    dp_peers = [(lax.rem(my_dp + k, ndp), my_tp) for k in range(1, ndp)]
    tp_peers = [(my_dp, lax.rem(my_tp + k, ntp)) for k in range(1, ntp)]
    for peer in dp_peers + tp_peers:
        pl.semaphore_signal(barrier, inc=1, device_id=peer, device_id_type=MESH)

    @pl.when(owning)
    def _():
        each_other(lambda device: pl.semaphore_signal(barrier, inc=1, device_id=device, device_id_type=MESH))

    grams[my_tp] = jnp.zeros(grams.shape[1:], jnp.float32)

    def left_copy(q, peer):
        return pltpu.make_async_remote_copy(
            src_ref=lefts.at[q, my_dp], dst_ref=lefts.at[q, my_dp],
            send_sem=left_send, recv_sem=left_recv.at[q],
            device_id=peer, device_id_type=MESH,
        )

    basis_load.wait()
    for load in loads:
        load.wait()
    own_left = [
        lax.dot_general(
            b_buf[l].astype(jnp.bfloat16), g_buf[l], (((1,), (1,)), ((), ())), preferred_element_type=jnp.float32
        )
        for l in range(layers)
    ]
    for q in range(layers // 2):
        lefts[q, my_dp] = pack(own_left[2 * q:2 * q + 2])
    pl.semaphore_wait(barrier, ndp - 1 + ntp - 1 + pieces - jnp.where(owning, 1, 0))
    for q in range(layers // 2):
        for peer in dp_peers:
            left_copy(q, peer).start()

    def part_copy(j):
        return pltpu.make_async_remote_copy(
            src_ref=rights.at[j], dst_ref=parts.at[me],
            send_sem=part_send, recv_sem=part_recv,
            device_id=owners[j], device_id_type=MESH,
        )

    all_left = []
    for q in range(layers // 2):
        landed = lefts.at[q, pl.ds(0, ndp - 1)]
        pltpu.make_async_copy(landed, landed, left_recv.at[q]).wait()
        both = lefts[q, 0]
        for d in range(1, ndp):
            both = both + lefts[q, d]
        for l, left in zip((2 * q, 2 * q + 1), unpack(both)):
            all_left.append(left)
            right = jnp.dot(left.astype(jnp.bfloat16), g_buf[l], preferred_element_type=jnp.float32)
            for t in range(tiles):
                rights[l * tiles + t] = right[:, t * LANES:(t + 1) * LANES]
        for j in range(2 * q * tiles, (2 * q + 2) * tiles):

            @pl.when(jnp.logical_not(is_me(owners[j])))
            def _():
                part_copy(j).start()

    stacked = jnp.concatenate(all_left, axis=0)
    products = lax.dot_general(
        stacked, stacked, (((1,), (1,)), ((), ())),
        precision=lax.Precision.HIGHEST, preferred_element_type=jnp.float32,
    )
    where = lax.broadcasted_iota(jnp.int32, (rank, layers * rank), 1) // rank
    packed = jnp.zeros((rank, layers * rank), jnp.float32)
    for l in range(layers):
        packed = jnp.where(where == l, products[l * rank:(l + 1) * rank], packed)
    grams[my_tp, :, :layers * rank] = packed

    def gram_copy(peer):
        return pltpu.make_async_remote_copy(
            src_ref=grams.at[my_tp], dst_ref=grams.at[my_tp],
            send_sem=gram_send, recv_sem=gram_recv,
            device_id=peer, device_id_type=MESH,
        )

    for peer in tp_peers:
        gram_copy(peer).start()

    def full_copy(device):
        return pltpu.make_async_remote_copy(
            src_ref=full.at[my_piece], dst_ref=full.at[my_piece],
            send_sem=full_send, recv_sem=full_recv.at[my_layer],
            device_id=device, device_id_type=MESH,
        )

    @pl.when(owning)
    def _():
        landed = parts.at[pl.ds(0, n - 1)]
        pltpu.make_async_copy(landed, landed, part_recv).wait()
        parts[me] = rights[my_piece]
        sums = [parts[i] for i in range(8)]
        for i in range(8, n):
            sums[i % 8] = sums[i % 8] + parts[i]
        while len(sums) > 1:
            sums = [a + b for a, b in zip(sums[::2], sums[1::2])]
        full[my_piece] = sums[0]
        each_other(lambda device: full_copy(device).start())

    landed_grams = grams.at[pl.ds(0, ntp - 1)]
    pltpu.make_async_copy(landed_grams, landed_grams, gram_recv).wait()
    gram_sum = jnp.sum(grams[...], axis=0)
    line = lax.broadcasted_iota(jnp.int32, (rank, rank), 0)
    diagonal = line == lax.broadcasted_iota(jnp.int32, (rank, rank), 1)
    step_line = lax.broadcasted_iota(jnp.int32, (rank, 1), 0)
    systems = []
    for l in range(layers):
        gram = gram_sum[:, l * rank:(l + 1) * rank]
        ridge = 0.001 * (jnp.sum(jnp.where(diagonal, gram, 0.0)) / rank)
        systems.append((gram + jnp.where(diagonal, ridge, 0.0), all_left[l]))
    for k in range(rank):
        after = []
        for gram, y in systems:
            pivot = 1.0 / gram[k:k + 1, k:k + 1]
            gram_row, y_row = gram[k:k + 1] * pivot, y[k:k + 1] * pivot
            factor = gram[:, k:k + 1]
            here = step_line == k
            after.append((
                jnp.where(here, gram_row, gram - factor * gram_row),
                jnp.where(here, y_row, y - factor * y_row),
            ))
        systems = after
    for l in range(layers):
        high, mid, low = split3(systems[l][1] / ndp)
        y = jnp.concatenate([high, high, high, mid, mid, low], axis=0)
        y_buf[l] = y.T.astype(jnp.bfloat16)
    for load in state_loads:
        load.wait()

    start = first_tile(my_dp, jnp.minimum)
    shift = lax.rem(span * LANES - (my_dp * columns - start * LANES), span * LANES)

    def wait_full(l, count):
        landed = full.at[pl.ds(l * tiles, count)]
        pltpu.make_async_copy(landed, landed, full_recv.at[l]).wait()

    for l in range(layers):
        own_layer = owning & (my_layer == l)

        @pl.when(own_layer)
        def _():
            wait_full(l, tiles - 1)

        @pl.when(jnp.logical_not(own_layer))
        def _():
            wait_full(l, tiles)

        near = jnp.concatenate([full[l * tiles + start + i] for i in range(span)], axis=1)
        own = pltpu.roll(near, shift, 1)[:, :columns]
        high, mid, low = split3(own)
        own = jnp.concatenate([high, mid, low, high, mid, high], axis=0).astype(jnp.bfloat16)
        change = jnp.dot(y_buf[l], own, preferred_element_type=jnp.float32)
        moved = 0.9 * m_buf[l] + change
        out_momentum[l] = moved
        out_weights[l] = w_buf[l] - 0.02 * moved
        right = jnp.concatenate([full[l * tiles + t] for t in range(tiles)], axis=1)
        out_basis[l] = right * lax.rsqrt(jnp.mean(right * right) + 1e-12)

    for q in range(layers // 2):
        sent = lefts.at[q, pl.ds(0, ndp - 1)]
        pltpu.make_async_copy(sent, sent, left_send).wait()
    pltpu.make_async_copy(landed_grams, landed_grams, gram_send).wait()

    @pl.when(owning)
    def _():
        sent = rights.at[pl.ds(0, pieces - 1)]
        pltpu.make_async_copy(sent, sent, part_send).wait()
        sent = parts.at[pl.ds(0, n - 1)]
        pltpu.make_async_copy(sent, sent, full_send).wait()

    @pl.when(jnp.logical_not(owning))
    def _():
        sent = rights.at[pl.ds(0, pieces)]
        pltpu.make_async_copy(sent, sent, part_send).wait()


def writer(*refs):
    half = (len(refs) - 1) // 2
    copies = [pltpu.make_async_copy(refs[i], refs[half + i], refs[-1].at[i]) for i in range(half)]
    for copy in copies:
        copy.start()
    for copy in copies:
        copy.wait()


def solution(mesh):
    ndp, ntp = mesh.shape["dp"], mesh.shape["tp"]
    n = ndp * ntp

    def on_device(gradients, right_factor, weights_before, momentum):
        layers, rows, width = gradients.shape[1:]
        rank = right_factor.shape[2]
        columns = weights_before.shape[2]
        pieces = layers * (width // LANES)
        basis = jnp.swapaxes(right_factor, 1, 2)
        f32 = jnp.float32
        keep = functools.partial(pltpu.with_memory_space_constraint, memory_space=pltpu.HBM)
        results = pl.pallas_call(
            functools.partial(kernel, ndp, ntp),
            out_shape=(
                jax.ShapeDtypeStruct((layers, rows, columns), f32),
                jax.ShapeDtypeStruct((layers, rank, width), f32),
                jax.ShapeDtypeStruct((layers, rows, columns), f32),
            ),
            in_specs=[
                pl.BlockSpec(memory_space=pltpu.HBM),
                pl.BlockSpec(memory_space=pltpu.HBM),
                pl.BlockSpec(memory_space=pltpu.HBM),
                pl.BlockSpec(memory_space=pltpu.HBM),
            ],
            out_specs=[pl.BlockSpec(memory_space=pltpu.VMEM)] * 3,
            scratch_shapes=[
                pltpu.VMEM((layers, rank, width), f32),
                pltpu.VMEM((layers, rows, width), jnp.bfloat16),
                pltpu.VMEM((layers, rows, columns), f32),
                pltpu.VMEM((layers, rows, columns), f32),
                pltpu.VMEM((layers // 2, ndp, rank, 2 * rows), f32),
                pltpu.VMEM((ntp, rank, LANES), f32),
                pltpu.VMEM((pieces, rank, LANES), f32),
                pltpu.VMEM((n, rank, LANES), f32),
                pltpu.VMEM((pieces, rank, LANES), f32),
                pltpu.VMEM((layers, rows, 6 * rank), jnp.bfloat16),
                pltpu.SemaphoreType.DMA((layers,)),
                pltpu.SemaphoreType.DMA((3,)),
                pltpu.SemaphoreType.DMA,
                pltpu.SemaphoreType.DMA((layers // 2,)),
                pltpu.SemaphoreType.DMA,
                pltpu.SemaphoreType.DMA,
                pltpu.SemaphoreType.DMA,
                pltpu.SemaphoreType.DMA,
                pltpu.SemaphoreType.DMA,
                pltpu.SemaphoreType.DMA((layers,)),
            ],
            compiler_params=pltpu.CompilerParams(
                collective_id=0, has_side_effects=True, vmem_limit_bytes=24 * 1024 * 1024
            ),
        )(
            keep(gradients[0]), keep(basis),
            keep(weights_before), keep(momentum),
        )
        new_weights, new_basis, new_momentum = pl.pallas_call(
            writer,
            out_shape=tuple(jax.ShapeDtypeStruct(x.shape, x.dtype) for x in results),
            in_specs=[pl.BlockSpec(memory_space=pltpu.VMEM)] * 3,
            out_specs=[pl.BlockSpec(memory_space=pltpu.HBM)] * 3,
            scratch_shapes=[pltpu.SemaphoreType.DMA((3,))],
        )(*(pltpu.with_memory_space_constraint(x, pltpu.VMEM) for x in results))
        return new_weights, jnp.swapaxes(new_basis, 1, 2), new_momentum

    in_specs = (P("dp", None, "tp", None), P(), P(None, "tp", "dp"), P(None, "tp", "dp"))
    out_specs = (P(None, "tp", "dp"), P(), P(None, "tp", "dp"))
    return jax.shard_map(on_device, mesh=mesh, in_specs=in_specs, out_specs=out_specs, check_vma=False)
```

```python
import functools

import jax
import jax.numpy as jnp
from jax import lax
from jax.experimental import pallas as pl
from jax.experimental.pallas import tpu as pltpu
from jax.sharding import PartitionSpec as P

MESH = pl.DeviceIdType.MESH
LANES = 128


def split3(x):
    high = x.astype(jnp.bfloat16).astype(jnp.float32)
    rest = x - high
    mid = rest.astype(jnp.bfloat16).astype(jnp.float32)
    low = (rest - mid).astype(jnp.bfloat16).astype(jnp.float32)
    return high, mid, low


def pack(pair):
    whole = pair[0].shape[1] // LANES * LANES
    return jnp.concatenate([x[:, :whole] for x in pair] + [x[:, whole:] for x in pair], axis=1)


def unpack(x):
    rows = x.shape[1] // 2
    whole = rows // LANES * LANES
    rest = rows - whole
    return [
        jnp.concatenate(
            [x[:, i * whole:(i + 1) * whole], x[:, 2 * whole + i * rest:2 * whole + (i + 1) * rest]], axis=1
        )
        for i in range(2)
    ]


def owner_place(j):
    x_hi, y, z = j % 2, j // 2 % 4, j // 8
    return y * 2 + (y + z) % 2, z * 4 + x_hi * 2 + 1


def start_order(device):
    dp, tp = device
    x, y, z, core = tp // 2 % 2 * 2 + dp % 2, dp // 2, tp // 4, tp % 2
    return 10 * z + 6 * y + 4 * x + 5 * (1 - core)


def kernel(
    ndp, ntp, grads, basis, weights, momentum,
    out_weights, out_basis, out_momentum,
    b_buf, g_buf, w_buf, m_buf, lefts, grams, rights, parts, full, y_buf,
    g_sem, wm_sem, left_send, left_recv, gram_send, gram_recv, part_send, part_recv, full_send, full_recv,
    ready, go,
):
    layers, rows, width = grads.shape
    rank = basis.shape[1]
    columns = weights.shape[2]
    n = ndp * ntp
    tiles = width // LANES
    pieces = layers * tiles
    my_dp, my_tp = lax.axis_index("dp"), lax.axis_index("tp")
    me = my_dp * ntp + my_tp

    span = max(
        ((d + 1) * columns - 1) // LANES - d * columns // LANES + 1 for d in range(ndp)
    )

    def first_tile(d, least=min):
        return least(d * columns // LANES, tiles - span)

    owners = [owner_place(j) for j in range(pieces)]
    devices = sorted(((d, p) for d in range(ndp) for p in range(ntp)), key=start_order)

    def is_me(device):
        return me == device[0] * ntp + device[1]

    hub = (0, ntp - 1)
    is_hub = is_me(hub)
    my_piece = jnp.int32(0)
    for j in range(1, pieces):
        my_piece = jnp.where(is_me(owners[j]), j, my_piece)
    owning = (my_piece > 0) | is_me(owners[0])
    my_layer = my_piece // tiles

    def each_other(act):
        for device in devices:
            if device in owners or device == hub:

                @pl.when(jnp.logical_not(is_me(device)))
                def _():
                    act(device)
            else:
                act(device)

    basis_load = pltpu.make_async_copy(basis, b_buf, wm_sem.at[2])
    basis_load.start()
    loads = [pltpu.make_async_copy(grads.at[l], g_buf.at[l], g_sem.at[l]) for l in range(layers)]
    for load in loads:
        load.start()
    state_loads = [
        pltpu.make_async_copy(weights, w_buf, wm_sem.at[0]),
        pltpu.make_async_copy(momentum, m_buf, wm_sem.at[1]),
    ]

    barrier = pltpu.get_barrier_semaphore()
    for k in range(1, ndp):

        @pl.when(k > my_dp)
        def _():
            pl.semaphore_signal(barrier, inc=1, device_id=(k, my_tp), device_id_type=MESH)

    @pl.when(jnp.logical_not(is_hub))
    def _():
        pl.semaphore_signal(barrier, inc=1, device_id=hub, device_id_type=MESH)

    @pl.when(my_dp > 0)
    def _():
        pl.semaphore_wait(barrier, my_dp)

    for k in range(ndp - 1):

        @pl.when(k < my_dp)
        def _():
            pl.semaphore_signal(ready.at[my_dp], inc=1, device_id=(k, my_tp), device_id_type=MESH)

    grams[my_tp] = jnp.zeros(grams.shape[1:], jnp.float32)

    def left_copy(q, k):
        return pltpu.make_async_remote_copy(
            src_ref=lefts.at[q, my_dp], dst_ref=lefts.at[q, my_dp],
            send_sem=left_send, recv_sem=left_recv.at[q],
            device_id=(k, my_tp), device_id_type=MESH,
        )

    basis_load.wait()
    for q in range(layers // 2):
        pair = (2 * q, 2 * q + 1)
        for l in pair:
            loads[l].wait()
        lefts[q, my_dp] = pack([
            lax.dot_general(
                b_buf[l].astype(jnp.bfloat16), g_buf[l], (((1,), (1,)), ((), ())), preferred_element_type=jnp.float32
            )
            for l in pair
        ])
        for k in range(ndp - 1):

            @pl.when(k < my_dp)
            def _():
                left_copy(q, k).start()
    for load in state_loads:
        load.start()
    for k in range(1, ndp):

        @pl.when(k > my_dp)
        def _():
            pl.semaphore_wait(ready.at[k], 1)
            for q in range(layers // 2):
                left_copy(q, k).start()

    @pl.when(is_hub)
    def _():
        pl.semaphore_wait(barrier, n - 1)
        each_other(lambda device: pl.semaphore_signal(go, inc=1, device_id=device, device_id_type=MESH))

    tp_peers = [(my_dp, lax.rem(my_tp + k, ntp)) for k in range(1, ntp)]

    def part_copy(j):
        return pltpu.make_async_remote_copy(
            src_ref=rights.at[j], dst_ref=parts.at[me],
            send_sem=part_send, recv_sem=part_recv,
            device_id=owners[j], device_id_type=MESH,
        )

    all_left = []
    for q in range(layers // 2):
        landed = lefts.at[q, pl.ds(0, ndp - 1)]
        pltpu.make_async_copy(landed, landed, left_recv.at[q]).wait()
        both = lefts[q, 0]
        for d in range(1, ndp):
            both = both + lefts[q, d]
        for l, left in zip((2 * q, 2 * q + 1), unpack(both)):
            all_left.append(left)
            right = jnp.dot(left.astype(jnp.bfloat16), g_buf[l], preferred_element_type=jnp.float32)
            for t in range(tiles):
                rights[l * tiles + t] = right[:, t * LANES:(t + 1) * LANES]
        if q == 0:

            @pl.when(jnp.logical_not(is_hub))
            def _():
                pl.semaphore_wait(go, 1)

        for j in range(2 * q * tiles, (2 * q + 2) * tiles):

            @pl.when(jnp.logical_not(is_me(owners[j])))
            def _():
                part_copy(j).start()

    stacked = jnp.concatenate(all_left, axis=0)
    products = lax.dot_general(
        stacked, stacked, (((1,), (1,)), ((), ())),
        precision=lax.Precision.HIGHEST, preferred_element_type=jnp.float32,
    )
    where = lax.broadcasted_iota(jnp.int32, (rank, layers * rank), 1) // rank
    packed = jnp.zeros((rank, layers * rank), jnp.float32)
    for l in range(layers):
        packed = jnp.where(where == l, products[l * rank:(l + 1) * rank], packed)
    grams[my_tp, :, :layers * rank] = packed

    def gram_copy(peer):
        return pltpu.make_async_remote_copy(
            src_ref=grams.at[my_tp], dst_ref=grams.at[my_tp],
            send_sem=gram_send, recv_sem=gram_recv,
            device_id=peer, device_id_type=MESH,
        )

    for peer in tp_peers:
        gram_copy(peer).start()

    def full_copy(device):
        return pltpu.make_async_remote_copy(
            src_ref=full.at[my_piece], dst_ref=full.at[my_piece],
            send_sem=full_send, recv_sem=full_recv.at[my_layer],
            device_id=device, device_id_type=MESH,
        )

    @pl.when(owning)
    def _():
        landed = parts.at[pl.ds(0, n - 1)]
        pltpu.make_async_copy(landed, landed, part_recv).wait()
        parts[me] = rights[my_piece]
        sums = [parts[i] for i in range(8)]
        for i in range(8, n):
            sums[i % 8] = sums[i % 8] + parts[i]
        while len(sums) > 1:
            sums = [a + b for a, b in zip(sums[::2], sums[1::2])]
        full[my_piece] = sums[0]
        each_other(lambda device: full_copy(device).start())

    landed_grams = grams.at[pl.ds(0, ntp - 1)]
    pltpu.make_async_copy(landed_grams, landed_grams, gram_recv).wait()
    gram_sum = jnp.sum(grams[...], axis=0)
    line = lax.broadcasted_iota(jnp.int32, (rank, rank), 0)
    diagonal = line == lax.broadcasted_iota(jnp.int32, (rank, rank), 1)
    step_line = lax.broadcasted_iota(jnp.int32, (rank, 1), 0)
    systems = []
    for l in range(layers):
        gram = gram_sum[:, l * rank:(l + 1) * rank]
        ridge = 0.001 * (jnp.sum(jnp.where(diagonal, gram, 0.0)) / rank)
        systems.append((gram + jnp.where(diagonal, ridge, 0.0), all_left[l]))
    for k in range(rank):
        after = []
        for gram, y in systems:
            pivot = 1.0 / gram[k:k + 1, k:k + 1]
            gram_row, y_row = gram[k:k + 1] * pivot, y[k:k + 1] * pivot
            factor = gram[:, k:k + 1]
            here = step_line == k
            after.append((
                jnp.where(here, gram_row, gram - factor * gram_row),
                jnp.where(here, y_row, y - factor * y_row),
            ))
        systems = after
    for l in range(layers):
        high, mid, low = split3(systems[l][1] / ndp)
        y = jnp.concatenate([high, high, high, mid, mid, low], axis=0)
        y_buf[l] = y.T.astype(jnp.bfloat16)
    for load in state_loads:
        load.wait()

    start = first_tile(my_dp, jnp.minimum)
    shift = lax.rem(span * LANES - (my_dp * columns - start * LANES), span * LANES)

    def wait_full(l, count):
        landed = full.at[pl.ds(l * tiles, count)]
        pltpu.make_async_copy(landed, landed, full_recv.at[l]).wait()

    for l in range(layers):
        own_layer = owning & (my_layer == l)

        @pl.when(own_layer)
        def _():
            wait_full(l, tiles - 1)

        @pl.when(jnp.logical_not(own_layer))
        def _():
            wait_full(l, tiles)

        near = jnp.concatenate([full[l * tiles + start + i] for i in range(span)], axis=1)
        own = pltpu.roll(near, shift, 1)[:, :columns]
        high, mid, low = split3(own)
        own = jnp.concatenate([high, mid, low, high, mid, high], axis=0).astype(jnp.bfloat16)
        change = jnp.dot(y_buf[l], own, preferred_element_type=jnp.float32)
        moved = 0.9 * m_buf[l] + change
        out_momentum[l] = moved
        out_weights[l] = w_buf[l] - 0.02 * moved
        right = jnp.concatenate([full[l * tiles + t] for t in range(tiles)], axis=1)
        out_basis[l] = right * lax.rsqrt(jnp.mean(right * right) + 1e-12)

    for q in range(layers // 2):
        sent = lefts.at[q, pl.ds(0, ndp - 1)]
        pltpu.make_async_copy(sent, sent, left_send).wait()
    pltpu.make_async_copy(landed_grams, landed_grams, gram_send).wait()

    @pl.when(owning)
    def _():
        sent = rights.at[pl.ds(0, pieces - 1)]
        pltpu.make_async_copy(sent, sent, part_send).wait()
        sent = parts.at[pl.ds(0, n - 1)]
        pltpu.make_async_copy(sent, sent, full_send).wait()

    @pl.when(jnp.logical_not(owning))
    def _():
        sent = rights.at[pl.ds(0, pieces)]
        pltpu.make_async_copy(sent, sent, part_send).wait()


def writer(*refs):
    half = (len(refs) - 1) // 2
    copies = [pltpu.make_async_copy(refs[i], refs[half + i], refs[-1].at[i]) for i in range(half)]
    for copy in copies:
        copy.start()
    for copy in copies:
        copy.wait()


def solution(mesh):
    ndp, ntp = mesh.shape["dp"], mesh.shape["tp"]
    n = ndp * ntp

    def on_device(gradients, right_factor, weights_before, momentum):
        layers, rows, width = gradients.shape[1:]
        rank = right_factor.shape[2]
        columns = weights_before.shape[2]
        pieces = layers * (width // LANES)
        basis = jnp.swapaxes(right_factor, 1, 2)
        f32 = jnp.float32
        keep = functools.partial(pltpu.with_memory_space_constraint, memory_space=pltpu.HBM)
        results = pl.pallas_call(
            functools.partial(kernel, ndp, ntp),
            out_shape=(
                jax.ShapeDtypeStruct((layers, rows, columns), f32),
                jax.ShapeDtypeStruct((layers, rank, width), f32),
                jax.ShapeDtypeStruct((layers, rows, columns), f32),
            ),
            in_specs=[
                pl.BlockSpec(memory_space=pltpu.HBM),
                pl.BlockSpec(memory_space=pltpu.HBM),
                pl.BlockSpec(memory_space=pltpu.HBM),
                pl.BlockSpec(memory_space=pltpu.HBM),
            ],
            out_specs=[pl.BlockSpec(memory_space=pltpu.VMEM)] * 3,
            scratch_shapes=[
                pltpu.VMEM((layers, rank, width), f32),
                pltpu.VMEM((layers, rows, width), jnp.bfloat16),
                pltpu.VMEM((layers, rows, columns), f32),
                pltpu.VMEM((layers, rows, columns), f32),
                pltpu.VMEM((layers // 2, ndp, rank, 2 * rows), f32),
                pltpu.VMEM((ntp, rank, LANES), f32),
                pltpu.VMEM((pieces, rank, LANES), f32),
                pltpu.VMEM((n, rank, LANES), f32),
                pltpu.VMEM((pieces, rank, LANES), f32),
                pltpu.VMEM((layers, rows, 6 * rank), jnp.bfloat16),
                pltpu.SemaphoreType.DMA((layers,)),
                pltpu.SemaphoreType.DMA((3,)),
                pltpu.SemaphoreType.DMA,
                pltpu.SemaphoreType.DMA((layers // 2,)),
                pltpu.SemaphoreType.DMA,
                pltpu.SemaphoreType.DMA,
                pltpu.SemaphoreType.DMA,
                pltpu.SemaphoreType.DMA,
                pltpu.SemaphoreType.DMA,
                pltpu.SemaphoreType.DMA((layers,)),
                pltpu.SemaphoreType.REGULAR((ndp,)),
                pltpu.SemaphoreType.REGULAR,
            ],
            compiler_params=pltpu.CompilerParams(
                collective_id=0, has_side_effects=True, vmem_limit_bytes=24 * 1024 * 1024
            ),
        )(
            keep(gradients[0]), keep(basis),
            keep(weights_before), keep(momentum),
        )
        new_weights, new_basis, new_momentum = pl.pallas_call(
            writer,
            out_shape=tuple(jax.ShapeDtypeStruct(x.shape, x.dtype) for x in results),
            in_specs=[pl.BlockSpec(memory_space=pltpu.VMEM)] * 3,
            out_specs=[pl.BlockSpec(memory_space=pltpu.HBM)] * 3,
            scratch_shapes=[pltpu.SemaphoreType.DMA((3,))],
        )(*(pltpu.with_memory_space_constraint(x, pltpu.VMEM) for x in results))
        return new_weights, jnp.swapaxes(new_basis, 1, 2), new_momentum

    in_specs = (P("dp", None, "tp", None), P(), P(None, "tp", "dp"), P(None, "tp", "dp"))
    out_specs = (P(None, "tp", "dp"), P(), P(None, "tp", "dp"))
    return jax.shard_map(on_device, mesh=mesh, in_specs=in_specs, out_specs=out_specs, check_vma=False)
```

```python
import functools

import jax
import jax.numpy as jnp
from jax import lax
from jax.experimental import pallas as pl
from jax.experimental.pallas import tpu as pltpu
from jax.sharding import PartitionSpec as P

MESH = pl.DeviceIdType.MESH
LANES = 128


def split3(x):
    high = x.astype(jnp.bfloat16).astype(jnp.float32)
    rest = x - high
    mid = rest.astype(jnp.bfloat16).astype(jnp.float32)
    low = (rest - mid).astype(jnp.bfloat16).astype(jnp.float32)
    return high, mid, low


def pack(pair):
    whole = pair[0].shape[1] // LANES * LANES
    return jnp.concatenate([x[:, :whole] for x in pair] + [x[:, whole:] for x in pair], axis=1)


def unpack(x):
    rows = x.shape[1] // 2
    whole = rows // LANES * LANES
    rest = rows - whole
    return [
        jnp.concatenate(
            [x[:, i * whole:(i + 1) * whole], x[:, 2 * whole + i * rest:2 * whole + (i + 1) * rest]], axis=1
        )
        for i in range(2)
    ]


def owner_place(j):
    x_hi, y, z = j % 2, j // 2 % 4, j // 8
    return y * 2 + (y + z) % 2, z * 4 + x_hi * 2 + 1


def start_order(device):
    dp, tp = device
    x, y, z, core = tp // 2 % 2 * 2 + dp % 2, dp // 2, tp // 4, tp % 2
    return 10 * z + 6 * y + 4 * x + 5 * (1 - core)


def kernel(
    ndp, ntp, grads, basis, weights, momentum,
    out_weights, out_basis, out_momentum,
    b_buf, g_buf, w_buf, m_buf, lefts, grams, rights, parts, full, y_buf,
    g_sem, wm_sem, left_send, left_recv, gram_send, gram_recv, part_send, part_recv, full_send, full_recv,
    go,
):
    layers, rows, width = grads.shape
    rank = basis.shape[1]
    columns = weights.shape[2]
    n = ndp * ntp
    tiles = width // LANES
    pieces = layers * tiles
    my_dp, my_tp = lax.axis_index("dp"), lax.axis_index("tp")
    me = my_dp * ntp + my_tp

    span = max(
        ((d + 1) * columns - 1) // LANES - d * columns // LANES + 1 for d in range(ndp)
    )

    def first_tile(d, least=min):
        return least(d * columns // LANES, tiles - span)

    owners = [owner_place(j) for j in range(pieces)]
    devices = sorted(((d, p) for d in range(ndp) for p in range(ntp)), key=start_order)

    def is_me(device):
        return me == device[0] * ntp + device[1]

    hub = (ndp - 2, ntp - 1)
    is_hub = is_me(hub)
    my_piece = jnp.int32(0)
    for j in range(1, pieces):
        my_piece = jnp.where(is_me(owners[j]), j, my_piece)
    owning = (my_piece > 0) | is_me(owners[0])
    my_layer = my_piece // tiles

    def each_other(act):
        for device in devices:
            if device in owners or device == hub:

                @pl.when(jnp.logical_not(is_me(device)))
                def _():
                    act(device)
            else:
                act(device)

    basis_load = pltpu.make_async_copy(basis, b_buf, wm_sem.at[2])
    basis_load.start()
    loads = [pltpu.make_async_copy(grads.at[l], g_buf.at[l], g_sem.at[l]) for l in range(layers)]
    for load in loads:
        load.start()
    state_loads = [
        pltpu.make_async_copy(weights, w_buf, wm_sem.at[0]),
        pltpu.make_async_copy(momentum, m_buf, wm_sem.at[1]),
    ]

    barrier = pltpu.get_barrier_semaphore()
    dp_peers = [(lax.rem(my_dp + k, ndp), my_tp) for k in range(1, ndp)]
    for peer in dp_peers:
        pl.semaphore_signal(barrier, inc=1, device_id=peer, device_id_type=MESH)

    @pl.when(my_tp != hub[1])
    def _():
        pl.semaphore_signal(barrier, inc=1, device_id=hub, device_id_type=MESH)

    grams[my_tp] = jnp.zeros(grams.shape[1:], jnp.float32)

    def left_copy(q, peer):
        return pltpu.make_async_remote_copy(
            src_ref=lefts.at[q, my_dp], dst_ref=lefts.at[q, my_dp],
            send_sem=left_send, recv_sem=left_recv.at[q],
            device_id=peer, device_id_type=MESH,
        )

    basis_load.wait()
    for q in range(layers // 2):
        pair = (2 * q, 2 * q + 1)
        for l in pair:
            loads[l].wait()
        lefts[q, my_dp] = pack([
            lax.dot_general(
                b_buf[l].astype(jnp.bfloat16), g_buf[l], (((1,), (1,)), ((), ())), preferred_element_type=jnp.float32
            )
            for l in pair
        ])
    for load in state_loads:
        load.start()
    pl.semaphore_wait(barrier, jnp.where(is_hub, n - 1, ndp - 1))
    for q in range(layers // 2):
        for peer in dp_peers:
            left_copy(q, peer).start()

    @pl.when(is_hub)
    def _():
        each_other(lambda device: pl.semaphore_signal(go, inc=1, device_id=device, device_id_type=MESH))

    tp_peers = [(my_dp, lax.rem(my_tp + k, ntp)) for k in range(1, ntp)]

    def part_copy(j):
        return pltpu.make_async_remote_copy(
            src_ref=rights.at[j], dst_ref=parts.at[me],
            send_sem=part_send, recv_sem=part_recv,
            device_id=owners[j], device_id_type=MESH,
        )

    all_left = []
    for q in range(layers // 2):
        landed = lefts.at[q, pl.ds(0, ndp - 1)]
        pltpu.make_async_copy(landed, landed, left_recv.at[q]).wait()
        both = lefts[q, 0]
        for d in range(1, ndp):
            both = both + lefts[q, d]
        for l, left in zip((2 * q, 2 * q + 1), unpack(both)):
            all_left.append(left)
            right = jnp.dot(left.astype(jnp.bfloat16), g_buf[l], preferred_element_type=jnp.float32)
            for t in range(tiles):
                rights[l * tiles + t] = right[:, t * LANES:(t + 1) * LANES]
        if q == 0:

            @pl.when(jnp.logical_not(is_hub))
            def _():
                pl.semaphore_wait(go, 1)

        for j in range(2 * q * tiles, (2 * q + 2) * tiles):

            @pl.when(jnp.logical_not(is_me(owners[j])))
            def _():
                part_copy(j).start()

    stacked = jnp.concatenate(all_left, axis=0)
    products = lax.dot_general(
        stacked, stacked, (((1,), (1,)), ((), ())),
        precision=lax.Precision.HIGHEST, preferred_element_type=jnp.float32,
    )
    where = lax.broadcasted_iota(jnp.int32, (rank, layers * rank), 1) // rank
    packed = jnp.zeros((rank, layers * rank), jnp.float32)
    for l in range(layers):
        packed = jnp.where(where == l, products[l * rank:(l + 1) * rank], packed)
    grams[my_tp, :, :layers * rank] = packed

    def gram_copy(peer):
        return pltpu.make_async_remote_copy(
            src_ref=grams.at[my_tp], dst_ref=grams.at[my_tp],
            send_sem=gram_send, recv_sem=gram_recv,
            device_id=peer, device_id_type=MESH,
        )

    for peer in tp_peers:
        gram_copy(peer).start()

    def full_copy(device):
        return pltpu.make_async_remote_copy(
            src_ref=full.at[my_piece], dst_ref=full.at[my_piece],
            send_sem=full_send, recv_sem=full_recv.at[my_layer],
            device_id=device, device_id_type=MESH,
        )

    @pl.when(owning)
    def _():
        landed = parts.at[pl.ds(0, n - 1)]
        pltpu.make_async_copy(landed, landed, part_recv).wait()
        parts[me] = rights[my_piece]
        sums = [parts[i] for i in range(8)]
        for i in range(8, n):
            sums[i % 8] = sums[i % 8] + parts[i]
        while len(sums) > 1:
            sums = [a + b for a, b in zip(sums[::2], sums[1::2])]
        full[my_piece] = sums[0]
        each_other(lambda device: full_copy(device).start())

    landed_grams = grams.at[pl.ds(0, ntp - 1)]
    pltpu.make_async_copy(landed_grams, landed_grams, gram_recv).wait()
    gram_sum = jnp.sum(grams[...], axis=0)
    line = lax.broadcasted_iota(jnp.int32, (rank, rank), 0)
    diagonal = line == lax.broadcasted_iota(jnp.int32, (rank, rank), 1)
    step_line = lax.broadcasted_iota(jnp.int32, (rank, 1), 0)
    systems = []
    for l in range(layers):
        gram = gram_sum[:, l * rank:(l + 1) * rank]
        ridge = 0.001 * (jnp.sum(jnp.where(diagonal, gram, 0.0)) / rank)
        systems.append((gram + jnp.where(diagonal, ridge, 0.0), all_left[l]))
    for k in range(rank):
        after = []
        for gram, y in systems:
            pivot = 1.0 / gram[k:k + 1, k:k + 1]
            gram_row, y_row = gram[k:k + 1] * pivot, y[k:k + 1] * pivot
            factor = gram[:, k:k + 1]
            here = step_line == k
            after.append((
                jnp.where(here, gram_row, gram - factor * gram_row),
                jnp.where(here, y_row, y - factor * y_row),
            ))
        systems = after
    for l in range(layers):
        high, mid, low = split3(systems[l][1] / ndp)
        y = jnp.concatenate([high, high, high, mid, mid, low], axis=0)
        y_buf[l] = y.T.astype(jnp.bfloat16)
    for load in state_loads:
        load.wait()

    start = first_tile(my_dp, jnp.minimum)
    shift = lax.rem(span * LANES - (my_dp * columns - start * LANES), span * LANES)

    def wait_full(l, count):
        landed = full.at[pl.ds(l * tiles, count)]
        pltpu.make_async_copy(landed, landed, full_recv.at[l]).wait()

    for l in range(layers):
        own_layer = owning & (my_layer == l)

        @pl.when(own_layer)
        def _():
            wait_full(l, tiles - 1)

        @pl.when(jnp.logical_not(own_layer))
        def _():
            wait_full(l, tiles)

        near = jnp.concatenate([full[l * tiles + start + i] for i in range(span)], axis=1)
        own = pltpu.roll(near, shift, 1)[:, :columns]
        high, mid, low = split3(own)
        own = jnp.concatenate([high, mid, low, high, mid, high], axis=0).astype(jnp.bfloat16)
        change = jnp.dot(y_buf[l], own, preferred_element_type=jnp.float32)
        moved = 0.9 * m_buf[l] + change
        out_momentum[l] = moved
        out_weights[l] = w_buf[l] - 0.02 * moved
        right = jnp.concatenate([full[l * tiles + t] for t in range(tiles)], axis=1)
        out_basis[l] = right * lax.rsqrt(jnp.mean(right * right) + 1e-12)

    for q in range(layers // 2):
        sent = lefts.at[q, pl.ds(0, ndp - 1)]
        pltpu.make_async_copy(sent, sent, left_send).wait()
    pltpu.make_async_copy(landed_grams, landed_grams, gram_send).wait()

    @pl.when(owning)
    def _():
        sent = rights.at[pl.ds(0, pieces - 1)]
        pltpu.make_async_copy(sent, sent, part_send).wait()
        sent = parts.at[pl.ds(0, n - 1)]
        pltpu.make_async_copy(sent, sent, full_send).wait()

    @pl.when(jnp.logical_not(owning))
    def _():
        sent = rights.at[pl.ds(0, pieces)]
        pltpu.make_async_copy(sent, sent, part_send).wait()


def writer(*refs):
    half = (len(refs) - 1) // 2
    copies = [pltpu.make_async_copy(refs[i], refs[half + i], refs[-1].at[i]) for i in range(half)]
    for copy in copies:
        copy.start()
    for copy in copies:
        copy.wait()


def solution(mesh):
    ndp, ntp = mesh.shape["dp"], mesh.shape["tp"]
    n = ndp * ntp

    def on_device(gradients, right_factor, weights_before, momentum):
        layers, rows, width = gradients.shape[1:]
        rank = right_factor.shape[2]
        columns = weights_before.shape[2]
        pieces = layers * (width // LANES)
        basis = jnp.swapaxes(right_factor, 1, 2)
        f32 = jnp.float32
        keep = functools.partial(pltpu.with_memory_space_constraint, memory_space=pltpu.HBM)
        results = pl.pallas_call(
            functools.partial(kernel, ndp, ntp),
            out_shape=(
                jax.ShapeDtypeStruct((layers, rows, columns), f32),
                jax.ShapeDtypeStruct((layers, rank, width), f32),
                jax.ShapeDtypeStruct((layers, rows, columns), f32),
            ),
            in_specs=[
                pl.BlockSpec(memory_space=pltpu.HBM),
                pl.BlockSpec(memory_space=pltpu.HBM),
                pl.BlockSpec(memory_space=pltpu.HBM),
                pl.BlockSpec(memory_space=pltpu.HBM),
            ],
            out_specs=[pl.BlockSpec(memory_space=pltpu.VMEM)] * 3,
            scratch_shapes=[
                pltpu.VMEM((layers, rank, width), f32),
                pltpu.VMEM((layers, rows, width), jnp.bfloat16),
                pltpu.VMEM((layers, rows, columns), f32),
                pltpu.VMEM((layers, rows, columns), f32),
                pltpu.VMEM((layers // 2, ndp, rank, 2 * rows), f32),
                pltpu.VMEM((ntp, rank, LANES), f32),
                pltpu.VMEM((pieces, rank, LANES), f32),
                pltpu.VMEM((n, rank, LANES), f32),
                pltpu.VMEM((pieces, rank, LANES), f32),
                pltpu.VMEM((layers, rows, 6 * rank), jnp.bfloat16),
                pltpu.SemaphoreType.DMA((layers,)),
                pltpu.SemaphoreType.DMA((3,)),
                pltpu.SemaphoreType.DMA,
                pltpu.SemaphoreType.DMA((layers // 2,)),
                pltpu.SemaphoreType.DMA,
                pltpu.SemaphoreType.DMA,
                pltpu.SemaphoreType.DMA,
                pltpu.SemaphoreType.DMA,
                pltpu.SemaphoreType.DMA,
                pltpu.SemaphoreType.DMA((layers,)),
                pltpu.SemaphoreType.REGULAR,
            ],
            compiler_params=pltpu.CompilerParams(
                collective_id=0, has_side_effects=True, vmem_limit_bytes=24 * 1024 * 1024
            ),
        )(
            keep(gradients[0]), keep(basis),
            keep(weights_before), keep(momentum),
        )
        new_weights, new_basis, new_momentum = pl.pallas_call(
            writer,
            out_shape=tuple(jax.ShapeDtypeStruct(x.shape, x.dtype) for x in results),
            in_specs=[pl.BlockSpec(memory_space=pltpu.VMEM)] * 3,
            out_specs=[pl.BlockSpec(memory_space=pltpu.HBM)] * 3,
            scratch_shapes=[pltpu.SemaphoreType.DMA((3,))],
        )(*(pltpu.with_memory_space_constraint(x, pltpu.VMEM) for x in results))
        return new_weights, jnp.swapaxes(new_basis, 1, 2), new_momentum

    in_specs = (P("dp", None, "tp", None), P(), P(None, "tp", "dp"), P(None, "tp", "dp"))
    out_specs = (P(None, "tp", "dp"), P(), P(None, "tp", "dp"))
    return jax.shard_map(on_device, mesh=mesh, in_specs=in_specs, out_specs=out_specs, check_vma=False)
```

```python
import functools

import jax
import jax.numpy as jnp
from jax import lax
from jax.experimental import pallas as pl
from jax.experimental.pallas import tpu as pltpu
from jax.sharding import PartitionSpec as P

MESH = pl.DeviceIdType.MESH
LANES = 128


def split3(x):
    high = x.astype(jnp.bfloat16).astype(jnp.float32)
    rest = x - high
    mid = rest.astype(jnp.bfloat16).astype(jnp.float32)
    low = (rest - mid).astype(jnp.bfloat16).astype(jnp.float32)
    return high, mid, low


def pack(pair):
    whole = pair[0].shape[1] // LANES * LANES
    return jnp.concatenate([x[:, :whole] for x in pair] + [x[:, whole:] for x in pair], axis=1)


def unpack(x):
    rows = x.shape[1] // 2
    whole = rows // LANES * LANES
    rest = rows - whole
    return [
        jnp.concatenate(
            [x[:, i * whole:(i + 1) * whole], x[:, 2 * whole + i * rest:2 * whole + (i + 1) * rest]], axis=1
        )
        for i in range(2)
    ]


OWNERS = [(0, 0, 0, 1), (0, 0, 3, 1), (3, 0, 0, 1), (2, 0, 0, 1), (1, 0, 0, 1), (0, 1, 0, 1), (0, 0, 1, 1), (0, 0, 2, 1), (0, 3, 0, 1), (3, 0, 3, 1), (2, 0, 3, 1), (0, 1, 3, 1), (1, 0, 3, 1), (0, 3, 3, 1), (0, 2, 0, 1), (3, 3, 0, 1), (2, 1, 0, 1), (1, 1, 0, 1), (3, 1, 0, 1), (3, 0, 1, 1), (3, 0, 2, 1), (1, 0, 1, 1), (2, 0, 1, 1), (1, 0, 2, 1)]


def owner_place(j):
    x, y, z, core = OWNERS[j]
    return y * 2 + x % 2, z * 4 + x // 2 * 2 + core


def start_order(device):
    dp, tp = device
    x, y, z, core = tp // 2 % 2 * 2 + dp % 2, dp // 2, tp // 4, tp % 2
    return 10 * z + 6 * y + 4 * x + 5 * (1 - core)


def kernel(
    ndp, ntp, grads, basis, weights, momentum,
    out_weights, out_basis, out_momentum,
    b_buf, g_buf, w_buf, m_buf, lefts, grams, rights, parts, full, y_buf,
    g_sem, wm_sem, left_send, left_recv, gram_send, gram_recv, part_send, part_recv, full_send, full_recv,
    go,
):
    layers, rows, width = grads.shape
    rank = basis.shape[1]
    columns = weights.shape[2]
    n = ndp * ntp
    tiles = width // LANES
    pieces = layers * tiles
    my_dp, my_tp = lax.axis_index("dp"), lax.axis_index("tp")
    me = my_dp * ntp + my_tp

    span = max(
        ((d + 1) * columns - 1) // LANES - d * columns // LANES + 1 for d in range(ndp)
    )

    def first_tile(d, least=min):
        return least(d * columns // LANES, tiles - span)

    owners = [owner_place(j) for j in range(pieces)]
    devices = sorted(((d, p) for d in range(ndp) for p in range(ntp)), key=start_order)

    def is_me(device):
        return me == device[0] * ntp + device[1]

    hub = (ndp - 2, ntp - 1)
    is_hub = is_me(hub)
    my_piece = jnp.int32(0)
    for j in range(1, pieces):
        my_piece = jnp.where(is_me(owners[j]), j, my_piece)
    owning = (my_piece > 0) | is_me(owners[0])
    my_layer = my_piece // tiles

    def each_other(act):
        for device in devices:
            if device in owners or device == hub:

                @pl.when(jnp.logical_not(is_me(device)))
                def _():
                    act(device)
            else:
                act(device)

    basis_load = pltpu.make_async_copy(basis, b_buf, wm_sem.at[2])
    basis_load.start()
    loads = [pltpu.make_async_copy(grads.at[l], g_buf.at[l], g_sem.at[l]) for l in range(layers)]
    for load in loads:
        load.start()
    state_loads = [
        pltpu.make_async_copy(weights, w_buf, wm_sem.at[0]),
        pltpu.make_async_copy(momentum, m_buf, wm_sem.at[1]),
    ]

    barrier = pltpu.get_barrier_semaphore()
    dp_peers = [(lax.rem(my_dp + k, ndp), my_tp) for k in range(1, ndp)]
    for peer in dp_peers:
        pl.semaphore_signal(barrier, inc=1, device_id=peer, device_id_type=MESH)

    @pl.when(my_tp != hub[1])
    def _():
        pl.semaphore_signal(barrier, inc=1, device_id=hub, device_id_type=MESH)

    grams[my_tp] = jnp.zeros(grams.shape[1:], jnp.float32)

    def left_copy(q, peer):
        return pltpu.make_async_remote_copy(
            src_ref=lefts.at[q, my_dp], dst_ref=lefts.at[q, my_dp],
            send_sem=left_send, recv_sem=left_recv.at[q],
            device_id=peer, device_id_type=MESH,
        )

    basis_load.wait()
    for q in range(layers // 2):
        pair = (2 * q, 2 * q + 1)
        for l in pair:
            loads[l].wait()
        lefts[q, my_dp] = pack([
            lax.dot_general(
                b_buf[l].astype(jnp.bfloat16), g_buf[l], (((1,), (1,)), ((), ())), preferred_element_type=jnp.float32
            )
            for l in pair
        ])
    for load in state_loads:
        load.start()
    pl.semaphore_wait(barrier, jnp.where(is_hub, n - 1, ndp - 1))
    for q in range(layers // 2):
        for peer in dp_peers:
            left_copy(q, peer).start()

    @pl.when(is_hub)
    def _():
        each_other(lambda device: pl.semaphore_signal(go, inc=1, device_id=device, device_id_type=MESH))

    tp_peers = [(my_dp, lax.rem(my_tp + k, ntp)) for k in range(1, ntp)]

    def part_copy(j):
        return pltpu.make_async_remote_copy(
            src_ref=rights.at[j], dst_ref=parts.at[me],
            send_sem=part_send, recv_sem=part_recv,
            device_id=owners[j], device_id_type=MESH,
        )

    all_left = []
    for q in range(layers // 2):
        landed = lefts.at[q, pl.ds(0, ndp - 1)]
        pltpu.make_async_copy(landed, landed, left_recv.at[q]).wait()
        both = lefts[q, 0]
        for d in range(1, ndp):
            both = both + lefts[q, d]
        for l, left in zip((2 * q, 2 * q + 1), unpack(both)):
            all_left.append(left)
            right = jnp.dot(left.astype(jnp.bfloat16), g_buf[l], preferred_element_type=jnp.float32)
            for t in range(tiles):
                rights[l * tiles + t] = right[:, t * LANES:(t + 1) * LANES]
        if q == 0:

            @pl.when(jnp.logical_not(is_hub))
            def _():
                pl.semaphore_wait(go, 1)

        for j in range(2 * q * tiles, (2 * q + 2) * tiles):

            @pl.when(jnp.logical_not(is_me(owners[j])))
            def _():
                part_copy(j).start()

    stacked = jnp.concatenate(all_left, axis=0)
    products = lax.dot_general(
        stacked, stacked, (((1,), (1,)), ((), ())),
        precision=lax.Precision.HIGHEST, preferred_element_type=jnp.float32,
    )
    where = lax.broadcasted_iota(jnp.int32, (rank, layers * rank), 1) // rank
    packed = jnp.zeros((rank, layers * rank), jnp.float32)
    for l in range(layers):
        packed = jnp.where(where == l, products[l * rank:(l + 1) * rank], packed)
    grams[my_tp, :, :layers * rank] = packed

    def gram_copy(peer):
        return pltpu.make_async_remote_copy(
            src_ref=grams.at[my_tp], dst_ref=grams.at[my_tp],
            send_sem=gram_send, recv_sem=gram_recv,
            device_id=peer, device_id_type=MESH,
        )

    for peer in tp_peers:
        gram_copy(peer).start()

    def full_copy(device):
        return pltpu.make_async_remote_copy(
            src_ref=full.at[my_piece], dst_ref=full.at[my_piece],
            send_sem=full_send, recv_sem=full_recv.at[my_layer],
            device_id=device, device_id_type=MESH,
        )

    @pl.when(owning)
    def _():
        landed = parts.at[pl.ds(0, n - 1)]
        pltpu.make_async_copy(landed, landed, part_recv).wait()
        parts[me] = rights[my_piece]
        sums = [parts[i] for i in range(8)]
        for i in range(8, n):
            sums[i % 8] = sums[i % 8] + parts[i]
        while len(sums) > 1:
            sums = [a + b for a, b in zip(sums[::2], sums[1::2])]
        full[my_piece] = sums[0]
        each_other(lambda device: full_copy(device).start())

    landed_grams = grams.at[pl.ds(0, ntp - 1)]
    pltpu.make_async_copy(landed_grams, landed_grams, gram_recv).wait()
    gram_sum = jnp.sum(grams[...], axis=0)
    line = lax.broadcasted_iota(jnp.int32, (rank, rank), 0)
    diagonal = line == lax.broadcasted_iota(jnp.int32, (rank, rank), 1)
    step_line = lax.broadcasted_iota(jnp.int32, (rank, 1), 0)
    systems = []
    for l in range(layers):
        gram = gram_sum[:, l * rank:(l + 1) * rank]
        ridge = 0.001 * (jnp.sum(jnp.where(diagonal, gram, 0.0)) / rank)
        systems.append((gram + jnp.where(diagonal, ridge, 0.0), all_left[l]))
    for k in range(rank):
        after = []
        for gram, y in systems:
            pivot = 1.0 / gram[k:k + 1, k:k + 1]
            gram_row, y_row = gram[k:k + 1] * pivot, y[k:k + 1] * pivot
            factor = gram[:, k:k + 1]
            here = step_line == k
            after.append((
                jnp.where(here, gram_row, gram - factor * gram_row),
                jnp.where(here, y_row, y - factor * y_row),
            ))
        systems = after
    for l in range(layers):
        high, mid, low = split3(systems[l][1] / ndp)
        y = jnp.concatenate([high, high, high, mid, mid, low], axis=0)
        y_buf[l] = y.T.astype(jnp.bfloat16)
    for load in state_loads:
        load.wait()

    start = first_tile(my_dp, jnp.minimum)
    shift = lax.rem(span * LANES - (my_dp * columns - start * LANES), span * LANES)

    def wait_full(l, count):
        landed = full.at[pl.ds(l * tiles, count)]
        pltpu.make_async_copy(landed, landed, full_recv.at[l]).wait()

    for l in range(layers):
        own_layer = owning & (my_layer == l)

        @pl.when(own_layer)
        def _():
            wait_full(l, tiles - 1)

        @pl.when(jnp.logical_not(own_layer))
        def _():
            wait_full(l, tiles)

        near = jnp.concatenate([full[l * tiles + start + i] for i in range(span)], axis=1)
        own = pltpu.roll(near, shift, 1)[:, :columns]
        high, mid, low = split3(own)
        own = jnp.concatenate([high, mid, low, high, mid, high], axis=0).astype(jnp.bfloat16)
        change = jnp.dot(y_buf[l], own, preferred_element_type=jnp.float32)
        moved = 0.9 * m_buf[l] + change
        out_momentum[l] = moved
        out_weights[l] = w_buf[l] - 0.02 * moved
        right = jnp.concatenate([full[l * tiles + t] for t in range(tiles)], axis=1)
        out_basis[l] = right * lax.rsqrt(jnp.mean(right * right) + 1e-12)

    for q in range(layers // 2):
        sent = lefts.at[q, pl.ds(0, ndp - 1)]
        pltpu.make_async_copy(sent, sent, left_send).wait()
    pltpu.make_async_copy(landed_grams, landed_grams, gram_send).wait()

    @pl.when(owning)
    def _():
        sent = rights.at[pl.ds(0, pieces - 1)]
        pltpu.make_async_copy(sent, sent, part_send).wait()
        sent = parts.at[pl.ds(0, n - 1)]
        pltpu.make_async_copy(sent, sent, full_send).wait()

    @pl.when(jnp.logical_not(owning))
    def _():
        sent = rights.at[pl.ds(0, pieces)]
        pltpu.make_async_copy(sent, sent, part_send).wait()


def writer(*refs):
    half = (len(refs) - 1) // 2
    copies = [pltpu.make_async_copy(refs[i], refs[half + i], refs[-1].at[i]) for i in range(half)]
    for copy in copies:
        copy.start()
    for copy in copies:
        copy.wait()


def solution(mesh):
    ndp, ntp = mesh.shape["dp"], mesh.shape["tp"]
    n = ndp * ntp

    def on_device(gradients, right_factor, weights_before, momentum):
        layers, rows, width = gradients.shape[1:]
        rank = right_factor.shape[2]
        columns = weights_before.shape[2]
        pieces = layers * (width // LANES)
        basis = jnp.swapaxes(right_factor, 1, 2)
        f32 = jnp.float32
        keep = functools.partial(pltpu.with_memory_space_constraint, memory_space=pltpu.HBM)
        results = pl.pallas_call(
            functools.partial(kernel, ndp, ntp),
            out_shape=(
                jax.ShapeDtypeStruct((layers, rows, columns), f32),
                jax.ShapeDtypeStruct((layers, rank, width), f32),
                jax.ShapeDtypeStruct((layers, rows, columns), f32),
            ),
            in_specs=[
                pl.BlockSpec(memory_space=pltpu.HBM),
                pl.BlockSpec(memory_space=pltpu.HBM),
                pl.BlockSpec(memory_space=pltpu.HBM),
                pl.BlockSpec(memory_space=pltpu.HBM),
            ],
            out_specs=[pl.BlockSpec(memory_space=pltpu.VMEM)] * 3,
            scratch_shapes=[
                pltpu.VMEM((layers, rank, width), f32),
                pltpu.VMEM((layers, rows, width), jnp.bfloat16),
                pltpu.VMEM((layers, rows, columns), f32),
                pltpu.VMEM((layers, rows, columns), f32),
                pltpu.VMEM((layers // 2, ndp, rank, 2 * rows), f32),
                pltpu.VMEM((ntp, rank, LANES), f32),
                pltpu.VMEM((pieces, rank, LANES), f32),
                pltpu.VMEM((n, rank, LANES), f32),
                pltpu.VMEM((pieces, rank, LANES), f32),
                pltpu.VMEM((layers, rows, 6 * rank), jnp.bfloat16),
                pltpu.SemaphoreType.DMA((layers,)),
                pltpu.SemaphoreType.DMA((3,)),
                pltpu.SemaphoreType.DMA,
                pltpu.SemaphoreType.DMA((layers // 2,)),
                pltpu.SemaphoreType.DMA,
                pltpu.SemaphoreType.DMA,
                pltpu.SemaphoreType.DMA,
                pltpu.SemaphoreType.DMA,
                pltpu.SemaphoreType.DMA,
                pltpu.SemaphoreType.DMA((layers,)),
                pltpu.SemaphoreType.REGULAR,
            ],
            compiler_params=pltpu.CompilerParams(
                collective_id=0, has_side_effects=True, vmem_limit_bytes=24 * 1024 * 1024
            ),
        )(
            keep(gradients[0]), keep(basis),
            keep(weights_before), keep(momentum),
        )
        new_weights, new_basis, new_momentum = pl.pallas_call(
            writer,
            out_shape=tuple(jax.ShapeDtypeStruct(x.shape, x.dtype) for x in results),
            in_specs=[pl.BlockSpec(memory_space=pltpu.VMEM)] * 3,
            out_specs=[pl.BlockSpec(memory_space=pltpu.HBM)] * 3,
            scratch_shapes=[pltpu.SemaphoreType.DMA((3,))],
        )(*(pltpu.with_memory_space_constraint(x, pltpu.VMEM) for x in results))
        return new_weights, jnp.swapaxes(new_basis, 1, 2), new_momentum

    in_specs = (P("dp", None, "tp", None), P(), P(None, "tp", "dp"), P(None, "tp", "dp"))
    out_specs = (P(None, "tp", "dp"), P(), P(None, "tp", "dp"))
    return jax.shard_map(on_device, mesh=mesh, in_specs=in_specs, out_specs=out_specs, check_vma=False)
```

```python
import functools

import jax
import jax.numpy as jnp
from jax import lax
from jax.experimental import pallas as pl
from jax.experimental.pallas import tpu as pltpu
from jax.sharding import PartitionSpec as P

MESH = pl.DeviceIdType.MESH
LANES = 128


def split3(x):
    high = x.astype(jnp.bfloat16).astype(jnp.float32)
    rest = x - high
    mid = rest.astype(jnp.bfloat16).astype(jnp.float32)
    low = (rest - mid).astype(jnp.bfloat16).astype(jnp.float32)
    return high, mid, low


def pack(pair):
    whole = pair[0].shape[1] // LANES * LANES
    return jnp.concatenate([x[:, :whole] for x in pair] + [x[:, whole:] for x in pair], axis=1)


def unpack(x):
    rows = x.shape[1] // 2
    whole = rows // LANES * LANES
    rest = rows - whole
    return [
        jnp.concatenate(
            [x[:, i * whole:(i + 1) * whole], x[:, 2 * whole + i * rest:2 * whole + (i + 1) * rest]], axis=1
        )
        for i in range(2)
    ]


OWNERS = [(0, 0, 0, 1), (0, 0, 3, 1), (3, 0, 0, 1), (2, 0, 0, 1), (1, 0, 0, 1), (0, 1, 0, 1), (0, 0, 1, 1), (0, 0, 2, 1), (0, 3, 0, 1), (3, 0, 3, 1), (2, 0, 3, 1), (0, 1, 3, 1), (1, 0, 3, 1), (0, 3, 3, 1), (0, 2, 0, 1), (3, 3, 0, 1), (2, 1, 0, 1), (1, 1, 0, 1), (3, 1, 0, 1), (3, 0, 1, 1), (3, 0, 2, 1), (1, 0, 1, 1), (2, 0, 1, 1), (1, 0, 2, 1)]


def owner_place(j):
    x, y, z, core = OWNERS[j]
    return y * 2 + x % 2, z * 4 + x // 2 * 2 + core


def start_order(device):
    dp, tp = device
    x, y, z, core = tp // 2 % 2 * 2 + dp % 2, dp // 2, tp // 4, tp % 2
    return 10 * z + 6 * y + 4 * x + 5 * (1 - core)


def kernel(
    ndp, ntp, grads, basis, weights, momentum,
    out_weights, out_basis, out_momentum,
    b_buf, g_buf, state, lefts, grams, rights, parts, full, y_buf,
    g_sem, b_sem, state_sem, send, left_recv, gram_recv, part_recv, full_send, full_recv, go,
):
    layers, rows, width = grads.shape
    rank = basis.shape[1]
    columns = weights.shape[2]
    n = ndp * ntp
    tiles = width // LANES
    pieces = layers * tiles
    my_dp, my_tp = lax.axis_index("dp"), lax.axis_index("tp")
    me = my_dp * ntp + my_tp

    span = max(
        ((d + 1) * columns - 1) // LANES - d * columns // LANES + 1 for d in range(ndp)
    )

    def first_tile(d, least=min):
        return least(d * columns // LANES, tiles - span)

    owners = [owner_place(j) for j in range(pieces)]
    devices = sorted(((d, p) for d in range(ndp) for p in range(ntp)), key=start_order)

    def is_me(device):
        return me == device[0] * ntp + device[1]

    hub = (ndp - 2, ntp - 1)
    is_hub = is_me(hub)
    my_piece = jnp.int32(0)
    for j in range(1, pieces):
        my_piece = jnp.where(is_me(owners[j]), j, my_piece)
    owning = (my_piece > 0) | is_me(owners[0])

    def each_other(act):
        for device in devices:
            if device in owners or device == hub:

                @pl.when(jnp.logical_not(is_me(device)))
                def _():
                    act(device)
            else:
                act(device)

    basis_load = pltpu.make_async_copy(basis, b_buf, b_sem)
    loads = [
        pltpu.make_async_copy(grads.at[l], g_buf.at[l], g_sem.at[l // 2]) for l in range(layers)
    ]
    for load in loads[:2]:
        load.start()
    basis_load.start()
    for load in loads[2:]:
        load.start()
    state_loads = [
        pltpu.make_async_copy(weights, state.at[0], state_sem),
        pltpu.make_async_copy(momentum, state.at[1], state_sem),
    ]

    barrier = pltpu.get_barrier_semaphore()
    dp_peers = [
        (lax.rem(my_dp // 2 + dy, ndp // 2) * 2 + lax.rem(my_dp + dx, 2), my_tp)
        for dy, dx in ((2, 1), (1, 1), (3, 1), (2, 0), (1, 0), (3, 0), (0, 1))
    ]
    for peer in dp_peers:
        pl.semaphore_signal(barrier, inc=1, device_id=peer, device_id_type=MESH)

    @pl.when(my_tp != hub[1])
    def _():
        pl.semaphore_signal(barrier, inc=1, device_id=hub, device_id_type=MESH)

    grams[my_tp] = jnp.zeros(grams.shape[1:], jnp.float32)

    def left_copy(q, peer):
        return pltpu.make_async_remote_copy(
            src_ref=lefts.at[q, my_dp], dst_ref=lefts.at[q, my_dp],
            send_sem=send, recv_sem=left_recv.at[q],
            device_id=peer, device_id_type=MESH,
        )

    basis_load.wait()
    for q in range(layers // 2):
        pair = (2 * q, 2 * q + 1)
        loaded = g_buf.at[pl.ds(2 * q, 2)]
        pltpu.make_async_copy(loaded, loaded, g_sem.at[q]).wait()
        lefts[q, my_dp] = pack([
            lax.dot_general(
                g_buf[l], b_buf[l].astype(jnp.bfloat16), (((1,), (1,)), ((), ())), preferred_element_type=jnp.float32
            ).T
            for l in pair
        ])
    for load in state_loads:
        load.start()
    pl.semaphore_wait(barrier, jnp.where(is_hub, n - 1, ndp - 1))
    for q in range(layers // 2):
        for peer in dp_peers:
            left_copy(q, peer).start()

    @pl.when(is_hub)
    def _():
        each_other(lambda device: pl.semaphore_signal(go, inc=1, device_id=device, device_id_type=MESH))

    tp_peers = [(my_dp, lax.rem(my_tp + k, ntp)) for k in range(1, ntp)]

    def part_copy(j):
        return pltpu.make_async_remote_copy(
            src_ref=rights.at[j], dst_ref=parts.at[me],
            send_sem=send, recv_sem=part_recv,
            device_id=owners[j], device_id_type=MESH,
        )

    all_left = []
    for q in range(layers // 2):
        landed = lefts.at[q, pl.ds(0, ndp - 1)]
        pltpu.make_async_copy(landed, landed, left_recv.at[q]).wait()
        both = lefts[q, 0]
        for d in range(1, ndp):
            both = both + lefts[q, d]
        for l, left in zip((2 * q, 2 * q + 1), unpack(both)):
            all_left.append(left)
            right = jnp.dot(left.astype(jnp.bfloat16), g_buf[l], preferred_element_type=jnp.float32)
            for t in range(tiles):
                rights[l * tiles + t] = right[:, t * LANES:(t + 1) * LANES]
        if q == 0:

            @pl.when(jnp.logical_not(is_hub))
            def _():
                pl.semaphore_wait(go, 1)

        for j in range(2 * q * tiles, (2 * q + 2) * tiles):

            @pl.when(jnp.logical_not(is_me(owners[j])))
            def _():
                part_copy(j).start()

    stacked = jnp.concatenate(all_left, axis=0)
    products = lax.dot_general(
        stacked, stacked, (((1,), (1,)), ((), ())),
        precision=lax.Precision.HIGHEST, preferred_element_type=jnp.float32,
    )
    where = lax.broadcasted_iota(jnp.int32, (rank, layers * rank), 1) // rank
    packed = jnp.zeros((rank, layers * rank), jnp.float32)
    for l in range(layers):
        packed = jnp.where(where == l, products[l * rank:(l + 1) * rank], packed)
    grams[my_tp, :, :layers * rank] = packed

    def gram_copy(peer):
        return pltpu.make_async_remote_copy(
            src_ref=grams.at[my_tp], dst_ref=grams.at[my_tp],
            send_sem=send, recv_sem=gram_recv,
            device_id=peer, device_id_type=MESH,
        )

    for peer in tp_peers:
        gram_copy(peer).start()

    def full_copy(device):
        return pltpu.make_async_remote_copy(
            src_ref=full.at[my_piece], dst_ref=full.at[my_piece],
            send_sem=full_send, recv_sem=full_recv,
            device_id=device, device_id_type=MESH,
        )

    @pl.when(owning)
    def _():
        landed = parts.at[pl.ds(0, n - 1)]
        pltpu.make_async_copy(landed, landed, part_recv).wait()
        parts[me] = rights[my_piece]
        sums = [parts[i] for i in range(8)]
        for i in range(8, n):
            sums[i % 8] = sums[i % 8] + parts[i]
        while len(sums) > 1:
            sums = [a + b for a, b in zip(sums[::2], sums[1::2])]
        full[my_piece] = sums[0]
        each_other(lambda device: full_copy(device).start())

    landed_grams = grams.at[pl.ds(0, ntp - 1)]
    pltpu.make_async_copy(landed_grams, landed_grams, gram_recv).wait()
    gram_sum = jnp.sum(grams[...], axis=0)
    line = lax.broadcasted_iota(jnp.int32, (rank, rank), 0)
    diagonal = line == lax.broadcasted_iota(jnp.int32, (rank, rank), 1)
    step_line = lax.broadcasted_iota(jnp.int32, (rank, 1), 0)
    systems = []
    for l in range(layers):
        gram = gram_sum[:, l * rank:(l + 1) * rank]
        ridge = 0.001 * (jnp.sum(jnp.where(diagonal, gram, 0.0)) / rank)
        systems.append((gram + jnp.where(diagonal, ridge, 0.0), all_left[l]))
    for k in range(rank):
        after = []
        for gram, y in systems:
            pivot = 1.0 / gram[k:k + 1, k:k + 1]
            gram_row, y_row = gram[k:k + 1] * pivot, y[k:k + 1] * pivot
            factor = gram[:, k:k + 1]
            here = step_line == k
            after.append((
                jnp.where(here, gram_row, gram - factor * gram_row),
                jnp.where(here, y_row, y - factor * y_row),
            ))
        systems = after
    for l in range(layers):
        high, mid, low = split3(systems[l][1] / ndp)
        y = jnp.concatenate([high, high, high, mid, mid, low], axis=0)
        y_buf[l] = y.T.astype(jnp.bfloat16)
    pltpu.make_async_copy(state, state, state_sem).wait()

    start = first_tile(my_dp, jnp.minimum)
    shift = lax.rem(span * LANES - (my_dp * columns - start * LANES), span * LANES)

    def wait_full(count):
        landed = full.at[pl.ds(0, count)]
        pltpu.make_async_copy(landed, landed, full_recv).wait()

    @pl.when(owning)
    def _():
        wait_full(pieces - 1)

    @pl.when(jnp.logical_not(owning))
    def _():
        wait_full(pieces)

    for l in range(layers):
        near = jnp.concatenate([full[l * tiles + start + b] for b in range(span)], axis=1)
        own = pltpu.roll(near, shift, 1)[:, :columns]
        high, mid, low = split3(own)
        own = jnp.concatenate([high, mid, low, high, mid, high], axis=0).astype(jnp.bfloat16)
        change = jnp.dot(y_buf[l], own, preferred_element_type=jnp.float32)
        moved = 0.9 * state[1, l] + change
        out_momentum[l] = moved
        out_weights[l] = state[0, l] - 0.02 * moved
        right = jnp.concatenate([full[l * tiles + t] for t in range(tiles)], axis=1)
        out_basis[l] = right * lax.rsqrt(jnp.mean(right * right) + 1e-12)

    tile_sends = layers // 2 * (ndp - 1) * lefts.shape[3] // LANES + ntp - 1 + pieces

    def wait_sent(count, sem):
        sent = parts.at[pl.ds(0, count)]
        pltpu.make_async_copy(sent, sent, sem).wait()

    @pl.when(owning)
    def _():
        wait_sent(tile_sends - 1, send)
        wait_sent(n - 1, full_send)

    @pl.when(jnp.logical_not(owning))
    def _():
        wait_sent(tile_sends, send)


def writer(*refs):
    half = (len(refs) - 1) // 2
    copies = [pltpu.make_async_copy(refs[i], refs[half + i], refs[-1].at[i]) for i in range(half)]
    for copy in copies:
        copy.start()
    for copy in copies:
        copy.wait()


def solution(mesh):
    ndp, ntp = mesh.shape["dp"], mesh.shape["tp"]
    n = ndp * ntp

    def on_device(gradients, right_factor, weights_before, momentum):
        layers, rows, width = gradients.shape[1:]
        rank = right_factor.shape[2]
        columns = weights_before.shape[2]
        pieces = layers * (width // LANES)
        basis = jnp.swapaxes(right_factor, 1, 2)
        f32 = jnp.float32
        keep = functools.partial(pltpu.with_memory_space_constraint, memory_space=pltpu.HBM)
        results = pl.pallas_call(
            functools.partial(kernel, ndp, ntp),
            out_shape=(
                jax.ShapeDtypeStruct((layers, rows, columns), f32),
                jax.ShapeDtypeStruct((layers, rank, width), f32),
                jax.ShapeDtypeStruct((layers, rows, columns), f32),
            ),
            in_specs=[
                pl.BlockSpec(memory_space=pltpu.HBM),
                pl.BlockSpec(memory_space=pltpu.HBM),
                pl.BlockSpec(memory_space=pltpu.HBM),
                pl.BlockSpec(memory_space=pltpu.HBM),
            ],
            out_specs=[pl.BlockSpec(memory_space=pltpu.VMEM)] * 3,
            scratch_shapes=[
                pltpu.VMEM((layers, rank, width), f32),
                pltpu.VMEM((layers, rows, width), jnp.bfloat16),
                pltpu.VMEM((2, layers, rows, columns), f32),
                pltpu.VMEM((layers // 2, ndp, rank, 2 * rows), f32),
                pltpu.VMEM((ntp, rank, LANES), f32),
                pltpu.VMEM((pieces, rank, LANES), f32),
                pltpu.VMEM((n, rank, LANES), f32),
                pltpu.VMEM((pieces, rank, LANES), f32),
                pltpu.VMEM((layers, rows, 6 * rank), jnp.bfloat16),
                pltpu.SemaphoreType.DMA((layers // 2,)),
                pltpu.SemaphoreType.DMA,
                pltpu.SemaphoreType.DMA,
                pltpu.SemaphoreType.DMA,
                pltpu.SemaphoreType.DMA((layers // 2,)),
                pltpu.SemaphoreType.DMA,
                pltpu.SemaphoreType.DMA,
                pltpu.SemaphoreType.DMA,
                pltpu.SemaphoreType.DMA,
                pltpu.SemaphoreType.REGULAR,
            ],
            compiler_params=pltpu.CompilerParams(
                collective_id=0, has_side_effects=True, vmem_limit_bytes=24 * 1024 * 1024
            ),
        )(
            keep(gradients[0]), keep(basis),
            keep(weights_before), keep(momentum),
        )
        new_weights, new_basis, new_momentum = pl.pallas_call(
            writer,
            out_shape=tuple(jax.ShapeDtypeStruct(x.shape, x.dtype) for x in results),
            in_specs=[pl.BlockSpec(memory_space=pltpu.VMEM)] * 3,
            out_specs=[pl.BlockSpec(memory_space=pltpu.HBM)] * 3,
            scratch_shapes=[pltpu.SemaphoreType.DMA((3,))],
        )(*(pltpu.with_memory_space_constraint(x, pltpu.VMEM) for x in results))
        return new_weights, jnp.swapaxes(new_basis, 1, 2), new_momentum

    in_specs = (P("dp", None, "tp", None), P(), P(None, "tp", "dp"), P(None, "tp", "dp"))
    out_specs = (P(None, "tp", "dp"), P(), P(None, "tp", "dp"))
    return jax.shard_map(on_device, mesh=mesh, in_specs=in_specs, out_specs=out_specs, check_vma=False)
```

```python
import functools

import jax
import jax.numpy as jnp
from jax import lax
from jax.experimental import pallas as pl
from jax.experimental.pallas import tpu as pltpu
from jax.sharding import PartitionSpec as P

MESH = pl.DeviceIdType.MESH
LANES = 128


def split3(x):
    high = x.astype(jnp.bfloat16).astype(jnp.float32)
    rest = x - high
    mid = rest.astype(jnp.bfloat16).astype(jnp.float32)
    low = (rest - mid).astype(jnp.bfloat16).astype(jnp.float32)
    return high, mid, low


def pack(pair):
    whole = pair[0].shape[1] // LANES * LANES
    return jnp.concatenate([x[:, :whole] for x in pair] + [x[:, whole:] for x in pair], axis=1)


def unpack(x):
    rows = x.shape[1] // 2
    whole = rows // LANES * LANES
    rest = rows - whole
    return [
        jnp.concatenate(
            [x[:, i * whole:(i + 1) * whole], x[:, 2 * whole + i * rest:2 * whole + (i + 1) * rest]], axis=1
        )
        for i in range(2)
    ]


OWNERS = [
    (0, 3, 1, 1), (0, 0, 3, 1), (3, 0, 0, 1), (2, 0, 0, 1),
    (1, 0, 0, 1), (0, 1, 0, 1), (0, 0, 1, 1), (0, 0, 2, 1),
    (0, 3, 0, 1), (3, 0, 3, 1), (2, 0, 3, 1), (0, 1, 3, 1),
    (1, 0, 3, 1), (1, 1, 1, 1), (0, 2, 0, 1), (1, 1, 3, 1),
    (0, 1, 2, 1), (1, 1, 0, 1), (3, 1, 0, 1), (3, 0, 1, 1),
    (0, 1, 1, 1), (1, 0, 1, 1), (2, 0, 1, 1), (1, 0, 2, 1),
]


def owner_place(j):
    x, y, z, core = OWNERS[j]
    return y * 2 + x % 2, z * 4 + x // 2 * 2 + core


def start_order(device):
    dp, tp = device
    x, y, z, core = tp // 2 % 2 * 2 + dp % 2, dp // 2, tp // 4, tp % 2
    return 10 * z + 6 * y + 4 * x + 5 * (1 - core)


def kernel(
    ndp, ntp, grads, basis, weights, momentum,
    out_weights, out_basis, out_momentum,
    b_buf, g_buf, state, lefts, grams, rights, parts, full, y_buf,
    g_sem, b_sem, state_sem, send, left_recv, gram_recv, part_recv, full_send, full_recv, go,
):
    layers, rows, width = grads.shape
    rank = basis.shape[1]
    columns = weights.shape[2]
    n = ndp * ntp
    tiles = width // LANES
    pieces = layers * tiles
    my_dp, my_tp = lax.axis_index("dp"), lax.axis_index("tp")
    me = my_dp * ntp + my_tp

    span = max(
        ((d + 1) * columns - 1) // LANES - d * columns // LANES + 1 for d in range(ndp)
    )

    def first_tile(d, least=min):
        return least(d * columns // LANES, tiles - span)

    owners = [owner_place(j) for j in range(pieces)]
    devices = sorted(((d, p) for d in range(ndp) for p in range(ntp)), key=start_order)

    def is_me(device):
        return me == device[0] * ntp + device[1]

    hub = (ndp - 2, ntp - 1)
    is_hub = is_me(hub)
    my_piece = jnp.int32(0)
    for j in range(1, pieces):
        my_piece = jnp.where(is_me(owners[j]), j, my_piece)
    owning = (my_piece > 0) | is_me(owners[0])

    def each_other(act):
        for device in devices:
            if device in owners or device == hub:

                @pl.when(jnp.logical_not(is_me(device)))
                def _():
                    act(device)
            else:
                act(device)

    basis_load = pltpu.make_async_copy(basis, b_buf, b_sem)
    loads = [
        pltpu.make_async_copy(grads.at[l], g_buf.at[l], g_sem.at[l // 2]) for l in range(layers)
    ]
    state_loads = [
        pltpu.make_async_copy(weights, state.at[0], state_sem),
        pltpu.make_async_copy(momentum, state.at[1], state_sem),
    ]

    barrier = pltpu.get_barrier_semaphore()
    dp_peers = [
        (lax.rem(my_dp // 2 + dy, ndp // 2) * 2 + lax.rem(my_dp + dx, 2), my_tp)
        for dy, dx in ((2, 1), (1, 1), (3, 1), (2, 0), (1, 0), (3, 0), (0, 1))
    ]
    for peer in dp_peers:
        pl.semaphore_signal(barrier, inc=1, device_id=peer, device_id_type=MESH)

    for load in loads[:2]:
        load.start()
    basis_load.start()
    for load in loads[2:]:
        load.start()

    @pl.when(my_tp != hub[1])
    def _():
        pl.semaphore_signal(barrier, inc=1, device_id=hub, device_id_type=MESH)

    grams[my_tp] = jnp.zeros(grams.shape[1:], jnp.float32)

    def left_copy(q, peer):
        return pltpu.make_async_remote_copy(
            src_ref=lefts.at[q, my_dp], dst_ref=lefts.at[q, my_dp],
            send_sem=send, recv_sem=left_recv.at[q],
            device_id=peer, device_id_type=MESH,
        )

    basis_load.wait()
    for q in range(layers // 2):
        pair = (2 * q, 2 * q + 1)
        loaded = g_buf.at[pl.ds(2 * q, 2)]
        pltpu.make_async_copy(loaded, loaded, g_sem.at[q]).wait()
        lefts[q, my_dp] = pack([
            lax.dot_general(
                g_buf[l], b_buf[l].astype(jnp.bfloat16), (((1,), (1,)), ((), ())), preferred_element_type=jnp.float32
            ).T
            for l in pair
        ])
    for load in state_loads:
        load.start()
    pl.semaphore_wait(barrier, jnp.where(is_hub, n - 1, ndp - 1))
    for q in range(layers // 2):
        for peer in dp_peers:
            left_copy(q, peer).start()

    @pl.when(is_hub)
    def _():
        each_other(lambda device: pl.semaphore_signal(go, inc=1, device_id=device, device_id_type=MESH))

    tp_peers = [(my_dp, lax.rem(my_tp + k, ntp)) for k in range(1, ntp)]

    def part_copy(j):
        return pltpu.make_async_remote_copy(
            src_ref=rights.at[j], dst_ref=parts.at[me],
            send_sem=send, recv_sem=part_recv,
            device_id=owners[j], device_id_type=MESH,
        )

    all_left = []
    for q in range(layers // 2):
        landed = lefts.at[q, pl.ds(0, ndp - 1)]
        pltpu.make_async_copy(landed, landed, left_recv.at[q]).wait()
        both = lefts[q, 0]
        for d in range(1, ndp):
            both = both + lefts[q, d]
        for l, left in zip((2 * q, 2 * q + 1), unpack(both)):
            all_left.append(left)
            right = jnp.dot(left.astype(jnp.bfloat16), g_buf[l], preferred_element_type=jnp.float32)
            for t in range(tiles):
                rights[l * tiles + t] = right[:, t * LANES:(t + 1) * LANES]
        if q == 0:

            @pl.when(jnp.logical_not(is_hub))
            def _():
                pl.semaphore_wait(go, 1)

        for j in range(2 * q * tiles, (2 * q + 2) * tiles):

            @pl.when(jnp.logical_not(is_me(owners[j])))
            def _():
                part_copy(j).start()

    stacked = jnp.concatenate(all_left, axis=0)
    products = lax.dot_general(
        stacked, stacked, (((1,), (1,)), ((), ())),
        precision=lax.Precision.HIGHEST, preferred_element_type=jnp.float32,
    )
    where = lax.broadcasted_iota(jnp.int32, (rank, layers * rank), 1) // rank
    packed = jnp.zeros((rank, layers * rank), jnp.float32)
    for l in range(layers):
        packed = jnp.where(where == l, products[l * rank:(l + 1) * rank], packed)
    grams[my_tp, :, :layers * rank] = packed

    def gram_copy(peer):
        return pltpu.make_async_remote_copy(
            src_ref=grams.at[my_tp], dst_ref=grams.at[my_tp],
            send_sem=send, recv_sem=gram_recv,
            device_id=peer, device_id_type=MESH,
        )

    for peer in tp_peers:
        gram_copy(peer).start()

    def full_copy(device):
        return pltpu.make_async_remote_copy(
            src_ref=full.at[my_piece], dst_ref=full.at[my_piece],
            send_sem=full_send, recv_sem=full_recv,
            device_id=device, device_id_type=MESH,
        )

    @pl.when(owning)
    def _():
        landed = parts.at[pl.ds(0, n - 1)]
        pltpu.make_async_copy(landed, landed, part_recv).wait()
        parts[me] = rights[my_piece]
        sums = [parts[i] for i in range(8)]
        for i in range(8, n):
            sums[i % 8] = sums[i % 8] + parts[i]
        while len(sums) > 1:
            sums = [a + b for a, b in zip(sums[::2], sums[1::2])]
        full[my_piece] = sums[0]
        each_other(lambda device: full_copy(device).start())

    landed_grams = grams.at[pl.ds(0, ntp - 1)]
    pltpu.make_async_copy(landed_grams, landed_grams, gram_recv).wait()
    gram_sum = jnp.sum(grams[...], axis=0)
    line = lax.broadcasted_iota(jnp.int32, (rank, rank), 0)
    diagonal = line == lax.broadcasted_iota(jnp.int32, (rank, rank), 1)
    step_line = lax.broadcasted_iota(jnp.int32, (rank, 1), 0)
    systems = []
    for l in range(layers):
        gram = gram_sum[:, l * rank:(l + 1) * rank]
        ridge = 0.001 * (jnp.sum(jnp.where(diagonal, gram, 0.0)) / rank)
        systems.append((gram + jnp.where(diagonal, ridge, 0.0), all_left[l]))
    for k in range(rank):
        after = []
        for gram, y in systems:
            pivot = 1.0 / gram[k:k + 1, k:k + 1]
            gram_row, y_row = gram[k:k + 1] * pivot, y[k:k + 1] * pivot
            factor = gram[:, k:k + 1]
            here = step_line == k
            after.append((
                jnp.where(here, gram_row, gram - factor * gram_row),
                jnp.where(here, y_row, y - factor * y_row),
            ))
        systems = after
    for l in range(layers):
        high, mid, low = split3(systems[l][1] / ndp)
        y = jnp.concatenate([high, high, high, mid, mid, low], axis=0)
        y_buf[l] = y.T.astype(jnp.bfloat16)
    pltpu.make_async_copy(state, state, state_sem).wait()

    start = first_tile(my_dp, jnp.minimum)
    shift = lax.rem(span * LANES - (my_dp * columns - start * LANES), span * LANES)

    def wait_full(count):
        landed = full.at[pl.ds(0, count)]
        pltpu.make_async_copy(landed, landed, full_recv).wait()

    @pl.when(owning)
    def _():
        wait_full(pieces - 1)

    @pl.when(jnp.logical_not(owning))
    def _():
        wait_full(pieces)

    for l in range(layers):
        near = jnp.concatenate([full[l * tiles + start + b] for b in range(span)], axis=1)
        own = pltpu.roll(near, shift, 1)[:, :columns]
        high, mid, low = split3(own)
        own = jnp.concatenate([high, mid, low, high, mid, high], axis=0).astype(jnp.bfloat16)
        change = jnp.dot(y_buf[l], own, preferred_element_type=jnp.float32)
        moved = 0.9 * state[1, l] + change
        out_momentum[l] = moved
        out_weights[l] = state[0, l] - 0.02 * moved
        right = jnp.concatenate([full[l * tiles + t] for t in range(tiles)], axis=1)
        out_basis[l] = right * lax.rsqrt(jnp.mean(right * right) + 1e-12)

    tile_sends = layers // 2 * (ndp - 1) * lefts.shape[3] // LANES + ntp - 1 + pieces

    def wait_sent(count, sem):
        sent = parts.at[pl.ds(0, count)]
        pltpu.make_async_copy(sent, sent, sem).wait()

    @pl.when(owning)
    def _():
        wait_sent(tile_sends - 1, send)
        wait_sent(n - 1, full_send)

    @pl.when(jnp.logical_not(owning))
    def _():
        wait_sent(tile_sends, send)


def writer(*refs):
    half = (len(refs) - 1) // 2
    copies = [pltpu.make_async_copy(refs[i], refs[half + i], refs[-1].at[i]) for i in range(half)]
    for copy in copies:
        copy.start()
    for copy in copies:
        copy.wait()


def solution(mesh):
    ndp, ntp = mesh.shape["dp"], mesh.shape["tp"]
    n = ndp * ntp

    def on_device(gradients, right_factor, weights_before, momentum):
        layers, rows, width = gradients.shape[1:]
        rank = right_factor.shape[2]
        columns = weights_before.shape[2]
        pieces = layers * (width // LANES)
        basis = jnp.swapaxes(right_factor, 1, 2)
        f32 = jnp.float32
        keep = functools.partial(pltpu.with_memory_space_constraint, memory_space=pltpu.HBM)
        results = pl.pallas_call(
            functools.partial(kernel, ndp, ntp),
            out_shape=(
                jax.ShapeDtypeStruct((layers, rows, columns), f32),
                jax.ShapeDtypeStruct((layers, rank, width), f32),
                jax.ShapeDtypeStruct((layers, rows, columns), f32),
            ),
            in_specs=[
                pl.BlockSpec(memory_space=pltpu.HBM),
                pl.BlockSpec(memory_space=pltpu.HBM),
                pl.BlockSpec(memory_space=pltpu.HBM),
                pl.BlockSpec(memory_space=pltpu.HBM),
            ],
            out_specs=[pl.BlockSpec(memory_space=pltpu.VMEM)] * 3,
            scratch_shapes=[
                pltpu.VMEM((layers, rank, width), f32),
                pltpu.VMEM((layers, rows, width), jnp.bfloat16),
                pltpu.VMEM((2, layers, rows, columns), f32),
                pltpu.VMEM((layers // 2, ndp, rank, 2 * rows), f32),
                pltpu.VMEM((ntp, rank, LANES), f32),
                pltpu.VMEM((pieces, rank, LANES), f32),
                pltpu.VMEM((n, rank, LANES), f32),
                pltpu.VMEM((pieces, rank, LANES), f32),
                pltpu.VMEM((layers, rows, 6 * rank), jnp.bfloat16),
                pltpu.SemaphoreType.DMA((layers // 2,)),
                pltpu.SemaphoreType.DMA,
                pltpu.SemaphoreType.DMA,
                pltpu.SemaphoreType.DMA,
                pltpu.SemaphoreType.DMA((layers // 2,)),
                pltpu.SemaphoreType.DMA,
                pltpu.SemaphoreType.DMA,
                pltpu.SemaphoreType.DMA,
                pltpu.SemaphoreType.DMA,
                pltpu.SemaphoreType.REGULAR,
            ],
            compiler_params=pltpu.CompilerParams(
                collective_id=0, has_side_effects=True, vmem_limit_bytes=24 * 1024 * 1024
            ),
        )(
            keep(gradients[0]), keep(basis),
            keep(weights_before), keep(momentum),
        )
        new_weights, new_basis, new_momentum = pl.pallas_call(
            writer,
            out_shape=tuple(jax.ShapeDtypeStruct(x.shape, x.dtype) for x in results),
            in_specs=[pl.BlockSpec(memory_space=pltpu.VMEM)] * 3,
            out_specs=[pl.BlockSpec(memory_space=pltpu.HBM)] * 3,
            scratch_shapes=[pltpu.SemaphoreType.DMA((3,))],
        )(*(pltpu.with_memory_space_constraint(x, pltpu.VMEM) for x in results))
        return new_weights, jnp.swapaxes(new_basis, 1, 2), new_momentum

    in_specs = (P("dp", None, "tp", None), P(), P(None, "tp", "dp"), P(None, "tp", "dp"))
    out_specs = (P(None, "tp", "dp"), P(), P(None, "tp", "dp"))
    return jax.shard_map(on_device, mesh=mesh, in_specs=in_specs, out_specs=out_specs, check_vma=False)
```

```python
import functools

import jax
import jax.numpy as jnp
from jax import lax
from jax.experimental import pallas as pl
from jax.experimental.pallas import tpu as pltpu
from jax.sharding import PartitionSpec as P

MESH = pl.DeviceIdType.MESH
LANES = 128


def split3(x):
    high = x.astype(jnp.bfloat16).astype(jnp.float32)
    rest = x - high
    mid = rest.astype(jnp.bfloat16).astype(jnp.float32)
    low = (rest - mid).astype(jnp.bfloat16).astype(jnp.float32)
    return high, mid, low


def pack(pair):
    whole = pair[0].shape[1] // LANES * LANES
    return jnp.concatenate([x[:, :whole] for x in pair] + [x[:, whole:] for x in pair], axis=1)


def unpack(x):
    rows = x.shape[1] // 2
    whole = rows // LANES * LANES
    rest = rows - whole
    return [
        jnp.concatenate(
            [x[:, i * whole:(i + 1) * whole], x[:, 2 * whole + i * rest:2 * whole + (i + 1) * rest]], axis=1
        )
        for i in range(2)
    ]


OWNERS = [
    (0, 3, 1, 1), (0, 0, 3, 1), (3, 0, 0, 1), (2, 0, 0, 1),
    (1, 0, 0, 1), (0, 1, 0, 1), (0, 0, 1, 1), (0, 0, 2, 1),
    (0, 3, 0, 1), (3, 0, 3, 1), (2, 0, 3, 1), (0, 1, 3, 1),
    (1, 0, 3, 1), (1, 1, 1, 1), (0, 2, 0, 1), (1, 1, 3, 1),
    (0, 1, 2, 1), (1, 1, 0, 1), (3, 1, 3, 1), (3, 0, 1, 1),
    (0, 1, 1, 1), (1, 0, 1, 1), (2, 0, 1, 1), (1, 0, 2, 1),
]


def owner_place(j):
    x, y, z, core = OWNERS[j]
    return y * 2 + x % 2, z * 4 + x // 2 * 2 + core


def start_order(device):
    dp, tp = device
    x, y, z, core = tp // 2 % 2 * 2 + dp % 2, dp // 2, tp // 4, tp % 2
    return 12 * z + 6 * y + 4 * x + 5 * (1 - core)


def kernel(
    ndp, ntp, grads, basis, weights, momentum,
    out_weights, out_basis, out_momentum,
    b_buf, g_buf, state, lefts, grams, rights, parts, full, y_buf,
    g_sem, b_sem, state_sem, send, left_recv, gram_recv, part_recv, full_send, full_recv, go,
):
    layers, rows, width = grads.shape
    rank = basis.shape[1]
    columns = weights.shape[2]
    n = ndp * ntp
    tiles = width // LANES
    pieces = layers * tiles
    my_dp, my_tp = lax.axis_index("dp"), lax.axis_index("tp")
    me = my_dp * ntp + my_tp

    span = max(
        ((d + 1) * columns - 1) // LANES - d * columns // LANES + 1 for d in range(ndp)
    )

    def first_tile(d, least=min):
        return least(d * columns // LANES, tiles - span)

    owners = [owner_place(j) for j in range(pieces)]
    devices = sorted(((d, p) for d in range(ndp) for p in range(ntp)), key=start_order)

    def is_me(device):
        return me == device[0] * ntp + device[1]

    hub = (ndp - 2, ntp - 1)
    is_hub = is_me(hub)
    my_piece = jnp.int32(0)
    for j in range(1, pieces):
        my_piece = jnp.where(is_me(owners[j]), j, my_piece)
    owning = (my_piece > 0) | is_me(owners[0])

    def each_other(act):
        for device in devices:
            if device in owners or device == hub:

                @pl.when(jnp.logical_not(is_me(device)))
                def _():
                    act(device)
            else:
                act(device)

    basis_load = pltpu.make_async_copy(basis, b_buf, b_sem)
    loads = [
        pltpu.make_async_copy(grads.at[l], g_buf.at[l], g_sem.at[l // 2]) for l in range(layers)
    ]
    state_loads = [
        pltpu.make_async_copy(weights, state.at[0], state_sem),
        pltpu.make_async_copy(momentum, state.at[1], state_sem),
    ]

    barrier = pltpu.get_barrier_semaphore()
    dp_peers = [
        (lax.rem(my_dp // 2 + dy, ndp // 2) * 2 + lax.rem(my_dp + dx, 2), my_tp)
        for dy, dx in ((2, 1), (1, 1), (3, 1), (2, 0), (1, 0), (3, 0), (0, 1))
    ]
    for peer in dp_peers:
        pl.semaphore_signal(barrier, inc=1, device_id=peer, device_id_type=MESH)

    for load in loads[:2]:
        load.start()
    basis_load.start()
    for load in loads[2:]:
        load.start()

    @pl.when(my_tp != hub[1])
    def _():
        pl.semaphore_signal(barrier, inc=1, device_id=hub, device_id_type=MESH)

    grams[my_tp] = jnp.zeros(grams.shape[1:], jnp.float32)

    def left_copy(q, peer):
        return pltpu.make_async_remote_copy(
            src_ref=lefts.at[q, my_dp], dst_ref=lefts.at[q, my_dp],
            send_sem=send, recv_sem=left_recv.at[q],
            device_id=peer, device_id_type=MESH,
        )

    basis_load.wait()
    for q in range(layers // 2):
        pair = (2 * q, 2 * q + 1)
        loaded = g_buf.at[pl.ds(2 * q, 2)]
        pltpu.make_async_copy(loaded, loaded, g_sem.at[q]).wait()
        lefts[q, my_dp] = pack([
            lax.dot_general(
                g_buf[l], b_buf[l].astype(jnp.bfloat16), (((1,), (1,)), ((), ())), preferred_element_type=jnp.float32
            ).T
            for l in pair
        ])
    for load in state_loads:
        load.start()
    pl.semaphore_wait(barrier, jnp.where(is_hub, n - 1, ndp - 1))
    for q in range(layers // 2):
        for peer in dp_peers:
            left_copy(q, peer).start()

    @pl.when(is_hub)
    def _():
        each_other(lambda device: pl.semaphore_signal(go, inc=1, device_id=device, device_id_type=MESH))

    tp_peers = [(my_dp, lax.rem(my_tp + k, ntp)) for k in range(1, ntp)]

    def part_copy(j):
        return pltpu.make_async_remote_copy(
            src_ref=rights.at[j], dst_ref=parts.at[me],
            send_sem=send, recv_sem=part_recv,
            device_id=owners[j], device_id_type=MESH,
        )

    all_left = []
    for q in range(layers // 2):
        landed = lefts.at[q, pl.ds(0, ndp - 1)]
        pltpu.make_async_copy(landed, landed, left_recv.at[q]).wait()
        both = lefts[q, 0]
        for d in range(1, ndp):
            both = both + lefts[q, d]
        for l, left in zip((2 * q, 2 * q + 1), unpack(both)):
            all_left.append(left)
            right = jnp.dot(left.astype(jnp.bfloat16), g_buf[l], preferred_element_type=jnp.float32)
            for t in range(tiles):
                rights[l * tiles + t] = right[:, t * LANES:(t + 1) * LANES]
        if q == 0:

            @pl.when(jnp.logical_not(is_hub))
            def _():
                pl.semaphore_wait(go, 1)

        for j in range(2 * q * tiles, (2 * q + 2) * tiles):

            @pl.when(jnp.logical_not(is_me(owners[j])))
            def _():
                part_copy(j).start()

    stacked = jnp.concatenate(all_left, axis=0)
    products = lax.dot_general(
        stacked, stacked, (((1,), (1,)), ((), ())),
        precision=lax.Precision.HIGHEST, preferred_element_type=jnp.float32,
    )
    where = lax.broadcasted_iota(jnp.int32, (rank, layers * rank), 1) // rank
    packed = jnp.zeros((rank, layers * rank), jnp.float32)
    for l in range(layers):
        packed = jnp.where(where == l, products[l * rank:(l + 1) * rank], packed)
    grams[my_tp, :, :layers * rank] = packed

    def gram_copy(peer):
        return pltpu.make_async_remote_copy(
            src_ref=grams.at[my_tp], dst_ref=grams.at[my_tp],
            send_sem=send, recv_sem=gram_recv,
            device_id=peer, device_id_type=MESH,
        )

    for peer in tp_peers:
        gram_copy(peer).start()

    def full_copy(device):
        return pltpu.make_async_remote_copy(
            src_ref=full.at[my_piece], dst_ref=full.at[my_piece],
            send_sem=full_send, recv_sem=full_recv,
            device_id=device, device_id_type=MESH,
        )

    @pl.when(owning)
    def _():
        landed = parts.at[pl.ds(0, n - 1)]
        pltpu.make_async_copy(landed, landed, part_recv).wait()
        parts[me] = rights[my_piece]
        sums = [parts[i] for i in range(8)]
        for i in range(8, n):
            sums[i % 8] = sums[i % 8] + parts[i]
        while len(sums) > 1:
            sums = [a + b for a, b in zip(sums[::2], sums[1::2])]
        full[my_piece] = sums[0]
        each_other(lambda device: full_copy(device).start())

    landed_grams = grams.at[pl.ds(0, ntp - 1)]
    pltpu.make_async_copy(landed_grams, landed_grams, gram_recv).wait()
    gram_sum = jnp.sum(grams[...], axis=0)
    line = lax.broadcasted_iota(jnp.int32, (rank, rank), 0)
    diagonal = line == lax.broadcasted_iota(jnp.int32, (rank, rank), 1)
    step_line = lax.broadcasted_iota(jnp.int32, (rank, 1), 0)
    systems = []
    for l in range(layers):
        gram = gram_sum[:, l * rank:(l + 1) * rank]
        ridge = 0.001 * (jnp.sum(jnp.where(diagonal, gram, 0.0)) / rank)
        systems.append((gram + jnp.where(diagonal, ridge, 0.0), all_left[l]))
    for k in range(rank):
        after = []
        for gram, y in systems:
            pivot = 1.0 / gram[k:k + 1, k:k + 1]
            gram_row, y_row = gram[k:k + 1] * pivot, y[k:k + 1] * pivot
            factor = gram[:, k:k + 1]
            here = step_line == k
            after.append((
                jnp.where(here, gram_row, gram - factor * gram_row),
                jnp.where(here, y_row, y - factor * y_row),
            ))
        systems = after
    for l in range(layers):
        high, mid, low = split3(systems[l][1] / ndp)
        y = jnp.concatenate([high, high, high, mid, mid, low], axis=0)
        y_buf[l] = y.T.astype(jnp.bfloat16)
    pltpu.make_async_copy(state, state, state_sem).wait()

    start = first_tile(my_dp, jnp.minimum)
    shift = lax.rem(span * LANES - (my_dp * columns - start * LANES), span * LANES)

    def wait_full(count):
        landed = full.at[pl.ds(0, count)]
        pltpu.make_async_copy(landed, landed, full_recv).wait()

    @pl.when(owning)
    def _():
        wait_full(pieces - 1)

    @pl.when(jnp.logical_not(owning))
    def _():
        wait_full(pieces)

    for l in range(layers):
        near = jnp.concatenate([full[l * tiles + start + b] for b in range(span)], axis=1)
        own = pltpu.roll(near, shift, 1)[:, :columns]
        high, mid, low = split3(own)
        own = jnp.concatenate([high, mid, low, high, mid, high], axis=0).astype(jnp.bfloat16)
        change = jnp.dot(y_buf[l], own, preferred_element_type=jnp.float32)
        moved = 0.9 * state[1, l] + change
        out_momentum[l] = moved
        out_weights[l] = state[0, l] - 0.02 * moved
        right = jnp.concatenate([full[l * tiles + t] for t in range(tiles)], axis=1)
        out_basis[l] = right * lax.rsqrt(jnp.mean(right * right) + 1e-12)

    tile_sends = layers // 2 * (ndp - 1) * lefts.shape[3] // LANES + ntp - 1 + pieces

    def wait_sent(count, sem):
        sent = parts.at[pl.ds(0, count)]
        pltpu.make_async_copy(sent, sent, sem).wait()

    @pl.when(owning)
    def _():
        wait_sent(tile_sends - 1, send)
        wait_sent(n - 1, full_send)

    @pl.when(jnp.logical_not(owning))
    def _():
        wait_sent(tile_sends, send)


def writer(*refs):
    half = (len(refs) - 1) // 2
    copies = [pltpu.make_async_copy(refs[i], refs[half + i], refs[-1].at[i]) for i in range(half)]
    for copy in copies:
        copy.start()
    for copy in copies:
        copy.wait()


def solution(mesh):
    ndp, ntp = mesh.shape["dp"], mesh.shape["tp"]
    n = ndp * ntp

    def on_device(gradients, right_factor, weights_before, momentum):
        layers, rows, width = gradients.shape[1:]
        rank = right_factor.shape[2]
        columns = weights_before.shape[2]
        pieces = layers * (width // LANES)
        basis = jnp.swapaxes(right_factor, 1, 2)
        f32 = jnp.float32
        keep = functools.partial(pltpu.with_memory_space_constraint, memory_space=pltpu.HBM)
        results = pl.pallas_call(
            functools.partial(kernel, ndp, ntp),
            out_shape=(
                jax.ShapeDtypeStruct((layers, rows, columns), f32),
                jax.ShapeDtypeStruct((layers, rank, width), f32),
                jax.ShapeDtypeStruct((layers, rows, columns), f32),
            ),
            in_specs=[
                pl.BlockSpec(memory_space=pltpu.HBM),
                pl.BlockSpec(memory_space=pltpu.HBM),
                pl.BlockSpec(memory_space=pltpu.HBM),
                pl.BlockSpec(memory_space=pltpu.HBM),
            ],
            out_specs=[pl.BlockSpec(memory_space=pltpu.VMEM)] * 3,
            scratch_shapes=[
                pltpu.VMEM((layers, rank, width), f32),
                pltpu.VMEM((layers, rows, width), jnp.bfloat16),
                pltpu.VMEM((2, layers, rows, columns), f32),
                pltpu.VMEM((layers // 2, ndp, rank, 2 * rows), f32),
                pltpu.VMEM((ntp, rank, LANES), f32),
                pltpu.VMEM((pieces, rank, LANES), f32),
                pltpu.VMEM((n, rank, LANES), f32),
                pltpu.VMEM((pieces, rank, LANES), f32),
                pltpu.VMEM((layers, rows, 6 * rank), jnp.bfloat16),
                pltpu.SemaphoreType.DMA((layers // 2,)),
                pltpu.SemaphoreType.DMA,
                pltpu.SemaphoreType.DMA,
                pltpu.SemaphoreType.DMA,
                pltpu.SemaphoreType.DMA((layers // 2,)),
                pltpu.SemaphoreType.DMA,
                pltpu.SemaphoreType.DMA,
                pltpu.SemaphoreType.DMA,
                pltpu.SemaphoreType.DMA,
                pltpu.SemaphoreType.REGULAR,
            ],
            compiler_params=pltpu.CompilerParams(
                collective_id=0, has_side_effects=True, vmem_limit_bytes=24 * 1024 * 1024
            ),
        )(
            keep(gradients[0]), keep(basis),
            keep(weights_before), keep(momentum),
        )
        new_weights, new_basis, new_momentum = pl.pallas_call(
            writer,
            out_shape=tuple(jax.ShapeDtypeStruct(x.shape, x.dtype) for x in results),
            in_specs=[pl.BlockSpec(memory_space=pltpu.VMEM)] * 3,
            out_specs=[pl.BlockSpec(memory_space=pltpu.HBM)] * 3,
            scratch_shapes=[pltpu.SemaphoreType.DMA((3,))],
        )(*(pltpu.with_memory_space_constraint(x, pltpu.VMEM) for x in results))
        return new_weights, jnp.swapaxes(new_basis, 1, 2), new_momentum

    in_specs = (P("dp", None, "tp", None), P(), P(None, "tp", "dp"), P(None, "tp", "dp"))
    out_specs = (P(None, "tp", "dp"), P(), P(None, "tp", "dp"))
    return jax.shard_map(on_device, mesh=mesh, in_specs=in_specs, out_specs=out_specs, check_vma=False)
```

```python
import functools

import jax
import jax.numpy as jnp
from jax import lax
from jax.experimental import pallas as pl
from jax.experimental.pallas import tpu as pltpu
from jax.sharding import PartitionSpec as P

MESH = pl.DeviceIdType.MESH
LANES = 128


def split3(x):
    high = x.astype(jnp.bfloat16).astype(jnp.float32)
    rest = x - high
    mid = rest.astype(jnp.bfloat16).astype(jnp.float32)
    low = (rest - mid).astype(jnp.bfloat16).astype(jnp.float32)
    return high, mid, low


def pack(pair):
    whole = pair[0].shape[1] // LANES * LANES
    return jnp.concatenate([x[:, :whole] for x in pair] + [x[:, whole:] for x in pair], axis=1)


def unpack(x):
    rows = x.shape[1] // 2
    whole = rows // LANES * LANES
    rest = rows - whole
    return [
        jnp.concatenate(
            [x[:, i * whole:(i + 1) * whole], x[:, 2 * whole + i * rest:2 * whole + (i + 1) * rest]], axis=1
        )
        for i in range(2)
    ]


OWNERS = [
    (0, 3, 1, 1), (0, 0, 3, 1), (3, 0, 0, 1), (2, 0, 0, 1),
    (1, 0, 0, 1), (0, 1, 0, 1), (0, 0, 1, 1), (0, 0, 2, 1),
    (0, 3, 0, 1), (3, 0, 3, 1), (2, 0, 3, 1), (0, 1, 3, 1),
    (1, 0, 3, 1), (1, 1, 1, 1), (0, 2, 0, 1), (1, 1, 3, 1),
    (0, 1, 2, 1), (1, 1, 0, 1), (3, 1, 3, 1), (3, 0, 1, 1),
    (0, 1, 1, 1), (1, 0, 1, 1), (2, 0, 1, 1), (1, 0, 2, 1),
]


def owner_place(j):
    x, y, z, core = OWNERS[j]
    return y * 2 + x % 2, z * 4 + x // 2 * 2 + core


def start_order(device):
    dp, tp = device
    x, y, z, core = tp // 2 % 2 * 2 + dp % 2, dp // 2, tp // 4, tp % 2
    return 12 * z + 6 * y + 4 * x + 5 * (1 - core)


def kernel(
    ndp, ntp, grads, basis, weights, momentum,
    out_weights, out_basis, out_momentum,
    b_buf, g_buf, state, lefts, grams, rights, parts, full, y_buf,
    g_sem, b_sem, state_sem, send, left_recv, gram_recv, part_recv, full_send, full_recv, go,
):
    layers, rows, width = grads.shape
    rank = basis.shape[1]
    columns = weights.shape[2]
    n = ndp * ntp
    tiles = width // LANES
    pieces = layers * tiles
    my_dp, my_tp = lax.axis_index("dp"), lax.axis_index("tp")
    me = my_dp * ntp + my_tp

    span = max(
        ((d + 1) * columns - 1) // LANES - d * columns // LANES + 1 for d in range(ndp)
    )

    def first_tile(d, least=min):
        return least(d * columns // LANES, tiles - span)

    owners = [owner_place(j) for j in range(pieces)]
    devices = sorted(((d, p) for d in range(ndp) for p in range(ntp)), key=start_order)

    def is_me(device):
        return me == device[0] * ntp + device[1]

    hub = (ndp - 2, ntp - 1)
    is_hub = is_me(hub)
    my_piece = jnp.int32(0)
    for j in range(1, pieces):
        my_piece = jnp.where(is_me(owners[j]), j, my_piece)
    owning = (my_piece > 0) | is_me(owners[0])

    def each_other(act):
        for device in devices:
            if device in owners or device == hub:

                @pl.when(jnp.logical_not(is_me(device)))
                def _():
                    act(device)
            else:
                act(device)

    basis_load = pltpu.make_async_copy(basis, b_buf, b_sem)
    loads = [
        pltpu.make_async_copy(grads.at[l], g_buf.at[l], g_sem.at[l // 2]) for l in range(layers)
    ]
    state_loads = [
        pltpu.make_async_copy(weights, state.at[0], state_sem),
        pltpu.make_async_copy(momentum, state.at[1], state_sem),
    ]

    barrier = pltpu.get_barrier_semaphore()
    dp_peers = [
        (lax.rem(my_dp // 2 + dy, ndp // 2) * 2 + lax.rem(my_dp + dx, 2), my_tp)
        for dy, dx in ((2, 1), (1, 1), (3, 1), (2, 0), (1, 0), (3, 0), (0, 1))
    ]
    for peer in dp_peers:
        pl.semaphore_signal(barrier, inc=1, device_id=peer, device_id_type=MESH)

    for load in loads[:2]:
        load.start()
    basis_load.start()
    for load in loads[2:]:
        load.start()

    @pl.when(my_tp != hub[1])
    def _():
        pl.semaphore_signal(barrier, inc=1, device_id=hub, device_id_type=MESH)

    grams[my_tp] = jnp.zeros(grams.shape[1:], jnp.float32)

    def left_copy(q, peer):
        return pltpu.make_async_remote_copy(
            src_ref=lefts.at[q, my_dp], dst_ref=lefts.at[q, my_dp],
            send_sem=send, recv_sem=left_recv.at[q],
            device_id=peer, device_id_type=MESH,
        )

    basis_load.wait()
    for q in range(layers // 2):
        pair = (2 * q, 2 * q + 1)
        loaded = g_buf.at[pl.ds(2 * q, 2)]
        pltpu.make_async_copy(loaded, loaded, g_sem.at[q]).wait()
        lefts[q, my_dp] = pack([
            lax.dot_general(
                b_buf[l].astype(jnp.bfloat16), g_buf[l], (((1,), (1,)), ((), ())), preferred_element_type=jnp.float32
            )
            for l in pair
        ])
    for load in state_loads:
        load.start()
    pl.semaphore_wait(barrier, jnp.where(is_hub, n - 1, ndp - 1))
    for q in range(layers // 2):
        for peer in dp_peers:
            left_copy(q, peer).start()

    @pl.when(is_hub)
    def _():
        each_other(lambda device: pl.semaphore_signal(go, inc=1, device_id=device, device_id_type=MESH))

    tp_peers = [(my_dp, lax.rem(my_tp + k, ntp)) for k in range(1, ntp)]

    def part_copy(j):
        return pltpu.make_async_remote_copy(
            src_ref=rights.at[j], dst_ref=parts.at[me],
            send_sem=send, recv_sem=part_recv,
            device_id=owners[j], device_id_type=MESH,
        )

    all_left = []
    for q in range(layers // 2):
        landed = lefts.at[q, pl.ds(0, ndp - 1)]
        pltpu.make_async_copy(landed, landed, left_recv.at[q]).wait()
        both = lefts[q, 0]
        for d in range(1, ndp):
            both = both + lefts[q, d]
        for l, left in zip((2 * q, 2 * q + 1), unpack(both)):
            all_left.append(left)
            right = jnp.dot(left.astype(jnp.bfloat16), g_buf[l], preferred_element_type=jnp.float32)
            for t in range(tiles):
                rights[l * tiles + t] = right[:, t * LANES:(t + 1) * LANES]
        if q == 0:

            @pl.when(jnp.logical_not(is_hub))
            def _():
                pl.semaphore_wait(go, 1)

        for j in range(2 * q * tiles, (2 * q + 2) * tiles):

            @pl.when(jnp.logical_not(is_me(owners[j])))
            def _():
                part_copy(j).start()

    stacked = jnp.concatenate(all_left, axis=0)
    products = lax.dot_general(
        stacked, stacked, (((1,), (1,)), ((), ())),
        precision=lax.Precision.HIGHEST, preferred_element_type=jnp.float32,
    )
    where = lax.broadcasted_iota(jnp.int32, (rank, layers * rank), 1) // rank
    packed = jnp.zeros((rank, layers * rank), jnp.float32)
    for l in range(layers):
        packed = jnp.where(where == l, products[l * rank:(l + 1) * rank], packed)
    grams[my_tp, :, :layers * rank] = packed

    def gram_copy(peer):
        return pltpu.make_async_remote_copy(
            src_ref=grams.at[my_tp], dst_ref=grams.at[my_tp],
            send_sem=send, recv_sem=gram_recv,
            device_id=peer, device_id_type=MESH,
        )

    for peer in tp_peers:
        gram_copy(peer).start()

    def full_copy(device):
        return pltpu.make_async_remote_copy(
            src_ref=full.at[my_piece], dst_ref=full.at[my_piece],
            send_sem=full_send, recv_sem=full_recv,
            device_id=device, device_id_type=MESH,
        )

    @pl.when(owning)
    def _():
        landed = parts.at[pl.ds(0, n - 1)]
        pltpu.make_async_copy(landed, landed, part_recv).wait()
        parts[me] = rights[my_piece]
        sums = [parts[i] for i in range(8)]
        for i in range(8, n):
            sums[i % 8] = sums[i % 8] + parts[i]
        while len(sums) > 1:
            sums = [a + b for a, b in zip(sums[::2], sums[1::2])]
        full[my_piece] = sums[0]
        each_other(lambda device: full_copy(device).start())

    landed_grams = grams.at[pl.ds(0, ntp - 1)]
    pltpu.make_async_copy(landed_grams, landed_grams, gram_recv).wait()
    gram_sum = jnp.sum(grams[...], axis=0)
    line = lax.broadcasted_iota(jnp.int32, (rank, rank), 0)
    diagonal = line == lax.broadcasted_iota(jnp.int32, (rank, rank), 1)
    step_line = lax.broadcasted_iota(jnp.int32, (rank, 1), 0)
    systems = []
    for l in range(layers):
        gram = gram_sum[:, l * rank:(l + 1) * rank]
        ridge = 0.001 * (jnp.sum(jnp.where(diagonal, gram, 0.0)) / rank)
        systems.append((gram + jnp.where(diagonal, ridge, 0.0), all_left[l]))
    for k in range(rank):
        after = []
        for gram, y in systems:
            pivot = 1.0 / gram[k:k + 1, k:k + 1]
            gram_row, y_row = gram[k:k + 1] * pivot, y[k:k + 1] * pivot
            factor = gram[:, k:k + 1]
            here = step_line == k
            after.append((
                jnp.where(here, gram_row, gram - factor * gram_row),
                jnp.where(here, y_row, y - factor * y_row),
            ))
        systems = after
    for l in range(layers):
        high, mid, low = split3(systems[l][1] / ndp)
        y = jnp.concatenate([high, high, high, mid, mid, low], axis=0)
        y_buf[l] = y.T.astype(jnp.bfloat16)
    pltpu.make_async_copy(state, state, state_sem).wait()

    start = first_tile(my_dp, jnp.minimum)
    shift = lax.rem(span * LANES - (my_dp * columns - start * LANES), span * LANES)

    def wait_full(count):
        landed = full.at[pl.ds(0, count)]
        pltpu.make_async_copy(landed, landed, full_recv).wait()

    @pl.when(owning)
    def _():
        wait_full(pieces - 1)

    @pl.when(jnp.logical_not(owning))
    def _():
        wait_full(pieces)

    for l in range(layers):
        near = jnp.concatenate([full[l * tiles + start + b] for b in range(span)], axis=1)
        own = pltpu.roll(near, shift, 1)[:, :columns]
        high, mid, low = split3(own)
        own = jnp.concatenate([high, mid, low, high, mid, high], axis=0).astype(jnp.bfloat16)
        change = jnp.dot(y_buf[l], own, preferred_element_type=jnp.float32)
        moved = 0.9 * state[1, l] + change
        out_momentum[l] = moved
        out_weights[l] = state[0, l] - 0.02 * moved
        right = jnp.concatenate([full[l * tiles + t] for t in range(tiles)], axis=1)
        out_basis[l] = right * lax.rsqrt(jnp.mean(right * right) + 1e-12)

    tile_sends = layers // 2 * (ndp - 1) * lefts.shape[3] // LANES + ntp - 1 + pieces

    def wait_sent(count, sem):
        sent = parts.at[pl.ds(0, count)]
        pltpu.make_async_copy(sent, sent, sem).wait()

    @pl.when(owning)
    def _():
        wait_sent(tile_sends - 1, send)
        wait_sent(n - 1, full_send)

    @pl.when(jnp.logical_not(owning))
    def _():
        wait_sent(tile_sends, send)


def writer(*refs):
    half = (len(refs) - 1) // 2
    copies = [pltpu.make_async_copy(refs[i], refs[half + i], refs[-1].at[i]) for i in range(half)]
    for copy in copies:
        copy.start()
    for copy in copies:
        copy.wait()


def solution(mesh):
    ndp, ntp = mesh.shape["dp"], mesh.shape["tp"]
    n = ndp * ntp

    def on_device(gradients, right_factor, weights_before, momentum):
        layers, rows, width = gradients.shape[1:]
        rank = right_factor.shape[2]
        columns = weights_before.shape[2]
        pieces = layers * (width // LANES)
        basis = jnp.swapaxes(right_factor, 1, 2)
        f32 = jnp.float32
        keep = functools.partial(pltpu.with_memory_space_constraint, memory_space=pltpu.HBM)
        results = pl.pallas_call(
            functools.partial(kernel, ndp, ntp),
            out_shape=(
                jax.ShapeDtypeStruct((layers, rows, columns), f32),
                jax.ShapeDtypeStruct((layers, rank, width), f32),
                jax.ShapeDtypeStruct((layers, rows, columns), f32),
            ),
            in_specs=[
                pl.BlockSpec(memory_space=pltpu.HBM),
                pl.BlockSpec(memory_space=pltpu.HBM),
                pl.BlockSpec(memory_space=pltpu.HBM),
                pl.BlockSpec(memory_space=pltpu.HBM),
            ],
            out_specs=[pl.BlockSpec(memory_space=pltpu.VMEM)] * 3,
            scratch_shapes=[
                pltpu.VMEM((layers, rank, width), f32),
                pltpu.VMEM((layers, rows, width), jnp.bfloat16),
                pltpu.VMEM((2, layers, rows, columns), f32),
                pltpu.VMEM((layers // 2, ndp, rank, 2 * rows), f32),
                pltpu.VMEM((ntp, rank, LANES), f32),
                pltpu.VMEM((pieces, rank, LANES), f32),
                pltpu.VMEM((n, rank, LANES), f32),
                pltpu.VMEM((pieces, rank, LANES), f32),
                pltpu.VMEM((layers, rows, 6 * rank), jnp.bfloat16),
                pltpu.SemaphoreType.DMA((layers // 2,)),
                pltpu.SemaphoreType.DMA,
                pltpu.SemaphoreType.DMA,
                pltpu.SemaphoreType.DMA,
                pltpu.SemaphoreType.DMA((layers // 2,)),
                pltpu.SemaphoreType.DMA,
                pltpu.SemaphoreType.DMA,
                pltpu.SemaphoreType.DMA,
                pltpu.SemaphoreType.DMA,
                pltpu.SemaphoreType.REGULAR,
            ],
            compiler_params=pltpu.CompilerParams(
                collective_id=0, has_side_effects=True, vmem_limit_bytes=24 * 1024 * 1024
            ),
        )(
            keep(gradients[0]), keep(basis),
            keep(weights_before), keep(momentum),
        )
        new_weights, new_basis, new_momentum = pl.pallas_call(
            writer,
            out_shape=tuple(jax.ShapeDtypeStruct(x.shape, x.dtype) for x in results),
            in_specs=[pl.BlockSpec(memory_space=pltpu.VMEM)] * 3,
            out_specs=[pl.BlockSpec(memory_space=pltpu.HBM)] * 3,
            scratch_shapes=[pltpu.SemaphoreType.DMA((3,))],
        )(*(pltpu.with_memory_space_constraint(x, pltpu.VMEM) for x in results))
        return new_weights, jnp.swapaxes(new_basis, 1, 2), new_momentum

    in_specs = (P("dp", None, "tp", None), P(), P(None, "tp", "dp"), P(None, "tp", "dp"))
    out_specs = (P(None, "tp", "dp"), P(), P(None, "tp", "dp"))
    return jax.shard_map(on_device, mesh=mesh, in_specs=in_specs, out_specs=out_specs, check_vma=False)
```

```python
import functools

import jax
import jax.numpy as jnp
from jax import lax
from jax.experimental import pallas as pl
from jax.experimental.pallas import tpu as pltpu
from jax.sharding import PartitionSpec as P

MESH = pl.DeviceIdType.MESH
LANES = 128


def split3(x):
    high = x.astype(jnp.bfloat16).astype(jnp.float32)
    rest = x - high
    mid = rest.astype(jnp.bfloat16).astype(jnp.float32)
    low = (rest - mid).astype(jnp.bfloat16).astype(jnp.float32)
    return high, mid, low


def pack(pair):
    whole = pair[0].shape[1] // LANES * LANES
    return jnp.concatenate([x[:, :whole] for x in pair] + [x[:, whole:] for x in pair], axis=1)


def unpack(x):
    rows = x.shape[1] // 2
    whole = rows // LANES * LANES
    rest = rows - whole
    return [
        jnp.concatenate(
            [x[:, i * whole:(i + 1) * whole], x[:, 2 * whole + i * rest:2 * whole + (i + 1) * rest]], axis=1
        )
        for i in range(2)
    ]


OWNERS = [
    (0, 3, 1, 1), (0, 0, 3, 1), (3, 0, 0, 1), (2, 0, 0, 1),
    (1, 0, 0, 1), (0, 1, 0, 1), (0, 0, 1, 1), (0, 0, 2, 1),
    (0, 3, 0, 1), (3, 0, 3, 1), (2, 0, 3, 1), (0, 1, 3, 1),
    (1, 0, 3, 1), (1, 1, 1, 1), (0, 2, 0, 1), (1, 1, 3, 1),
    (0, 1, 2, 1), (1, 1, 0, 1), (3, 1, 3, 1), (3, 0, 1, 1),
    (0, 1, 1, 1), (1, 0, 1, 1), (2, 0, 1, 1), (1, 0, 2, 1),
]


def owner_place(j):
    x, y, z, core = OWNERS[j]
    return y * 2 + x % 2, z * 4 + x // 2 * 2 + core


def start_order(device):
    dp, tp = device
    x, y, z, core = tp // 2 % 2 * 2 + dp % 2, dp // 2, tp // 4, tp % 2
    return 12 * z + 6 * y + 4 * x + 5 * (1 - core)


def kernel(
    ndp, ntp, grads, basis, weights, momentum,
    out_weights, out_basis, out_momentum,
    b_buf, g_buf, state, lefts, grams, rights, parts, full, y_buf,
    g_sem, b_sem, state_sem, send, left_recv, gram_recv, part_recv, full_send, full_recv, go,
):
    layers, rows, width = grads.shape
    rank = basis.shape[1]
    columns = weights.shape[2]
    n = ndp * ntp
    tiles = width // LANES
    pieces = layers * tiles
    my_dp, my_tp = lax.axis_index("dp"), lax.axis_index("tp")
    me = my_dp * ntp + my_tp

    span = max(
        ((d + 1) * columns - 1) // LANES - d * columns // LANES + 1 for d in range(ndp)
    )

    def first_tile(d, least=min):
        return least(d * columns // LANES, tiles - span)

    owners = [owner_place(j) for j in range(pieces)]
    devices = sorted(((d, p) for d in range(ndp) for p in range(ntp)), key=start_order)

    def is_me(device):
        return me == device[0] * ntp + device[1]

    hub = (ndp - 2, ntp - 1)
    is_hub = is_me(hub)
    my_piece = jnp.int32(0)
    for j in range(1, pieces):
        my_piece = jnp.where(is_me(owners[j]), j, my_piece)
    owning = (my_piece > 0) | is_me(owners[0])

    def each_other(act):
        for device in devices:
            if device in owners or device == hub:

                @pl.when(jnp.logical_not(is_me(device)))
                def _():
                    act(device)
            else:
                act(device)

    basis_load = pltpu.make_async_copy(basis, b_buf, b_sem)
    loads = [
        pltpu.make_async_copy(grads.at[l], g_buf.at[l], g_sem.at[l // 2]) for l in range(layers)
    ]
    state_loads = [
        pltpu.make_async_copy(weights, state.at[0], state_sem),
        pltpu.make_async_copy(momentum, state.at[1], state_sem),
    ]

    barrier = pltpu.get_barrier_semaphore()
    dp_peers = [
        (lax.rem(my_dp // 2 + dy, ndp // 2) * 2 + lax.rem(my_dp + dx, 2), my_tp)
        for dy, dx in ((2, 1), (1, 1), (3, 1), (2, 0), (1, 0), (3, 0), (0, 1))
    ]
    for peer in dp_peers:
        pl.semaphore_signal(barrier, inc=1, device_id=peer, device_id_type=MESH)

    for load in loads[:2]:
        load.start()
    basis_load.start()
    for load in loads[2:]:
        load.start()

    @pl.when(my_tp != hub[1])
    def _():
        pl.semaphore_signal(barrier, inc=1, device_id=hub, device_id_type=MESH)

    grams[my_tp] = jnp.zeros(grams.shape[1:], jnp.float32)

    def left_copy(q, peer):
        return pltpu.make_async_remote_copy(
            src_ref=lefts.at[q, my_dp], dst_ref=lefts.at[q, my_dp],
            send_sem=send, recv_sem=left_recv.at[q],
            device_id=peer, device_id_type=MESH,
        )

    basis_load.wait()
    for q in range(layers // 2):
        pair = (2 * q, 2 * q + 1)
        loaded = g_buf.at[pl.ds(2 * q, 2)]
        pltpu.make_async_copy(loaded, loaded, g_sem.at[q]).wait()
        lefts[q, my_dp] = pack([
            lax.dot_general(
                b_buf[l].astype(jnp.bfloat16), g_buf[l], (((1,), (1,)), ((), ())), preferred_element_type=jnp.float32
            )
            for l in pair
        ])
    pl.semaphore_wait(barrier, jnp.where(is_hub, n - 1, ndp - 1))
    for q in range(layers // 2):
        for peer in dp_peers:
            left_copy(q, peer).start()
    for load in state_loads:
        load.start()

    @pl.when(is_hub)
    def _():
        each_other(lambda device: pl.semaphore_signal(go, inc=1, device_id=device, device_id_type=MESH))

    tp_peers = [(my_dp, lax.rem(my_tp + k, ntp)) for k in range(1, ntp)]

    def part_copy(j):
        return pltpu.make_async_remote_copy(
            src_ref=rights.at[j], dst_ref=parts.at[me],
            send_sem=send, recv_sem=part_recv,
            device_id=owners[j], device_id_type=MESH,
        )

    all_left = []
    for q in range(layers // 2):
        landed = lefts.at[q, pl.ds(0, ndp - 1)]
        pltpu.make_async_copy(landed, landed, left_recv.at[q]).wait()
        both = lefts[q, 0]
        for d in range(1, ndp):
            both = both + lefts[q, d]
        for l, left in zip((2 * q, 2 * q + 1), unpack(both)):
            all_left.append(left)
            right = jnp.dot(left.astype(jnp.bfloat16), g_buf[l], preferred_element_type=jnp.float32)
            for t in range(tiles):
                rights[l * tiles + t] = right[:, t * LANES:(t + 1) * LANES]
        if q == 0:

            @pl.when(jnp.logical_not(is_hub))
            def _():
                pl.semaphore_wait(go, 1)

        for j in range(2 * q * tiles, (2 * q + 2) * tiles):

            @pl.when(jnp.logical_not(is_me(owners[j])))
            def _():
                part_copy(j).start()

    stacked = jnp.concatenate(all_left, axis=0)
    products = lax.dot_general(
        stacked, stacked, (((1,), (1,)), ((), ())),
        precision=lax.Precision.HIGHEST, preferred_element_type=jnp.float32,
    )
    where = lax.broadcasted_iota(jnp.int32, (rank, layers * rank), 1) // rank
    packed = jnp.zeros((rank, layers * rank), jnp.float32)
    for l in range(layers):
        packed = jnp.where(where == l, products[l * rank:(l + 1) * rank], packed)
    grams[my_tp, :, :layers * rank] = packed

    def gram_copy(peer):
        return pltpu.make_async_remote_copy(
            src_ref=grams.at[my_tp], dst_ref=grams.at[my_tp],
            send_sem=send, recv_sem=gram_recv,
            device_id=peer, device_id_type=MESH,
        )

    for peer in tp_peers:
        gram_copy(peer).start()

    def full_copy(device):
        return pltpu.make_async_remote_copy(
            src_ref=full.at[my_piece], dst_ref=full.at[my_piece],
            send_sem=full_send, recv_sem=full_recv,
            device_id=device, device_id_type=MESH,
        )

    @pl.when(owning)
    def _():
        landed = parts.at[pl.ds(0, n - 1)]
        pltpu.make_async_copy(landed, landed, part_recv).wait()
        parts[me] = rights[my_piece]
        sums = [parts[i] for i in range(8)]
        for i in range(8, n):
            sums[i % 8] = sums[i % 8] + parts[i]
        while len(sums) > 1:
            sums = [a + b for a, b in zip(sums[::2], sums[1::2])]
        full[my_piece] = sums[0]
        each_other(lambda device: full_copy(device).start())

    landed_grams = grams.at[pl.ds(0, ntp - 1)]
    pltpu.make_async_copy(landed_grams, landed_grams, gram_recv).wait()
    gram_sum = jnp.sum(grams[...], axis=0)
    line = lax.broadcasted_iota(jnp.int32, (rank, rank), 0)
    diagonal = line == lax.broadcasted_iota(jnp.int32, (rank, rank), 1)
    step_line = lax.broadcasted_iota(jnp.int32, (rank, 1), 0)
    systems = []
    for l in range(layers):
        gram = gram_sum[:, l * rank:(l + 1) * rank]
        ridge = 0.001 * (jnp.sum(jnp.where(diagonal, gram, 0.0)) / rank)
        systems.append((gram + jnp.where(diagonal, ridge, 0.0), all_left[l]))
    for k in range(rank):
        after = []
        for gram, y in systems:
            pivot = 1.0 / gram[k:k + 1, k:k + 1]
            gram_row, y_row = gram[k:k + 1] * pivot, y[k:k + 1] * pivot
            factor = gram[:, k:k + 1]
            here = step_line == k
            after.append((
                jnp.where(here, gram_row, gram - factor * gram_row),
                jnp.where(here, y_row, y - factor * y_row),
            ))
        systems = after
    for l in range(layers):
        high, mid, low = split3(systems[l][1] / ndp)
        y = jnp.concatenate([high, high, high, mid, mid, low], axis=0)
        y_buf[l] = y.T.astype(jnp.bfloat16)
    pltpu.make_async_copy(state, state, state_sem).wait()

    start = first_tile(my_dp, jnp.minimum)
    shift = lax.rem(span * LANES - (my_dp * columns - start * LANES), span * LANES)

    def wait_full(count):
        landed = full.at[pl.ds(0, count)]
        pltpu.make_async_copy(landed, landed, full_recv).wait()

    @pl.when(owning)
    def _():
        wait_full(pieces - 1)

    @pl.when(jnp.logical_not(owning))
    def _():
        wait_full(pieces)

    for l in range(layers):
        near = jnp.concatenate([full[l * tiles + start + b] for b in range(span)], axis=1)
        own = pltpu.roll(near, shift, 1)[:, :columns]
        high, mid, low = split3(own)
        own = jnp.concatenate([high, mid, low, high, mid, high], axis=0).astype(jnp.bfloat16)
        change = jnp.dot(y_buf[l], own, preferred_element_type=jnp.float32)
        moved = 0.9 * state[1, l] + change
        out_momentum[l] = moved
        out_weights[l] = state[0, l] - 0.02 * moved
        right = jnp.concatenate([full[l * tiles + t] for t in range(tiles)], axis=1)
        out_basis[l] = right * lax.rsqrt(jnp.mean(right * right) + 1e-12)

    tile_sends = layers // 2 * (ndp - 1) * lefts.shape[3] // LANES + ntp - 1 + pieces

    def wait_sent(count, sem):
        sent = parts.at[pl.ds(0, count)]
        pltpu.make_async_copy(sent, sent, sem).wait()

    @pl.when(owning)
    def _():
        wait_sent(tile_sends - 1, send)
        wait_sent(n - 1, full_send)

    @pl.when(jnp.logical_not(owning))
    def _():
        wait_sent(tile_sends, send)


def writer(*refs):
    half = (len(refs) - 1) // 2
    copies = [pltpu.make_async_copy(refs[i], refs[half + i], refs[-1].at[i]) for i in range(half)]
    for copy in copies:
        copy.start()
    for copy in copies:
        copy.wait()


def solution(mesh):
    ndp, ntp = mesh.shape["dp"], mesh.shape["tp"]
    n = ndp * ntp

    def on_device(gradients, right_factor, weights_before, momentum):
        layers, rows, width = gradients.shape[1:]
        rank = right_factor.shape[2]
        columns = weights_before.shape[2]
        pieces = layers * (width // LANES)
        basis = jnp.swapaxes(right_factor, 1, 2)
        f32 = jnp.float32
        keep = functools.partial(pltpu.with_memory_space_constraint, memory_space=pltpu.HBM)
        results = pl.pallas_call(
            functools.partial(kernel, ndp, ntp),
            out_shape=(
                jax.ShapeDtypeStruct((layers, rows, columns), f32),
                jax.ShapeDtypeStruct((layers, rank, width), f32),
                jax.ShapeDtypeStruct((layers, rows, columns), f32),
            ),
            in_specs=[
                pl.BlockSpec(memory_space=pltpu.HBM),
                pl.BlockSpec(memory_space=pltpu.HBM),
                pl.BlockSpec(memory_space=pltpu.HBM),
                pl.BlockSpec(memory_space=pltpu.HBM),
            ],
            out_specs=[pl.BlockSpec(memory_space=pltpu.VMEM)] * 3,
            scratch_shapes=[
                pltpu.VMEM((layers, rank, width), f32),
                pltpu.VMEM((layers, rows, width), jnp.bfloat16),
                pltpu.VMEM((2, layers, rows, columns), f32),
                pltpu.VMEM((layers // 2, ndp, rank, 2 * rows), f32),
                pltpu.VMEM((ntp, rank, LANES), f32),
                pltpu.VMEM((pieces, rank, LANES), f32),
                pltpu.VMEM((n, rank, LANES), f32),
                pltpu.VMEM((pieces, rank, LANES), f32),
                pltpu.VMEM((layers, rows, 6 * rank), jnp.bfloat16),
                pltpu.SemaphoreType.DMA((layers // 2,)),
                pltpu.SemaphoreType.DMA,
                pltpu.SemaphoreType.DMA,
                pltpu.SemaphoreType.DMA,
                pltpu.SemaphoreType.DMA((layers // 2,)),
                pltpu.SemaphoreType.DMA,
                pltpu.SemaphoreType.DMA,
                pltpu.SemaphoreType.DMA,
                pltpu.SemaphoreType.DMA,
                pltpu.SemaphoreType.REGULAR,
            ],
            compiler_params=pltpu.CompilerParams(
                collective_id=0, has_side_effects=True, vmem_limit_bytes=24 * 1024 * 1024
            ),
        )(
            keep(gradients[0]), keep(basis),
            keep(weights_before), keep(momentum),
        )
        new_weights, new_basis, new_momentum = pl.pallas_call(
            writer,
            out_shape=tuple(jax.ShapeDtypeStruct(x.shape, x.dtype) for x in results),
            in_specs=[pl.BlockSpec(memory_space=pltpu.VMEM)] * 3,
            out_specs=[pl.BlockSpec(memory_space=pltpu.HBM)] * 3,
            scratch_shapes=[pltpu.SemaphoreType.DMA((3,))],
        )(*(pltpu.with_memory_space_constraint(x, pltpu.VMEM) for x in results))
        return new_weights, jnp.swapaxes(new_basis, 1, 2), new_momentum

    in_specs = (P("dp", None, "tp", None), P(), P(None, "tp", "dp"), P(None, "tp", "dp"))
    out_specs = (P(None, "tp", "dp"), P(), P(None, "tp", "dp"))
    return jax.shard_map(on_device, mesh=mesh, in_specs=in_specs, out_specs=out_specs, check_vma=False)
```
